32 devices in a mesh: pipe: 4 (over x, core), expert: 4 (over z), tensor: 2 (over y).
Axes of the slice: x: 2, y: 2, z: 4, core: 2. Of those that a mesh axis runs over, the one named last changes fastest.
Arguments:
- stream: bfloat16 [2, 4, 64, 7168], P(None, 'pipe', 'expert', 'tensor'), may hold values from -6 to 6
- expert_ids: int32 [2, 4, 64, 2], P(None, 'pipe', 'expert'), may hold values from 0 to 3, all different within a row; in each aligned block of 16 rows (0 to 15, 16 to 31, ..., all dimensions but the last counted through in order) at most 12 rows name the same one
- norm_gain: float32 [4, 7168], P('pipe', 'tensor'), may hold values from 0.1 to 1.9
- router: float32 [4, 7168, 4], P('pipe', 'tensor'), may hold values from -0.0625 to 0.0625
- w_up: bfloat16 [4, 7168, 1024], P('expert', 'tensor'), may hold values from -0.0625 to 0.0625
- w_down: bfloat16 [4, 1024, 7168], P('expert', None, 'tensor'), may hold values from -0.1875 to 0.1875
Outputs:
- result: bfloat16 [2, 4, 64, 7168], P(None, 'pipe', 'expert', 'tensor')
The draws below stay inside these ranges and needn't reach their ends.
Inputs may be any that keep to these rules, and one draw needn't show every extreme that they name: `expert_ids`: each token names 2 different experts. Among the 16 tokens of one direction held by one index of the expert axis at one section, at most 12 name any one expert, and in every draw some expert is named by exactly 12 of them.
All inputs are finite; a program needn't handle non-finite values.
Results may differ from the reference program's by a relative error of at most 0.0065.
Values may be sent and summed in bfloat16 or wider, within the bound.
A program may use at most 64 MiB of HBM per device.

```python
import math
import jax
import jax.numpy as jnp
import numpy as np
from jax import lax

D = 7168
FF = 1024
TOK_DEV = 16
PIPE = 4
EXPERTS = 4
TOP = 2
TOKENS = 64
CAP = 12
N_EXPERT = 4


def shard_levels(stream_key, extent, split, smallest, top_value):
    factor_of, own = 1.0, jax.random.fold_in(stream_key, 6)
    for position, blocks in split:
        draws = jnp.exp(jax.random.uniform(jax.random.fold_in(own, position), (blocks,), jnp.float32, smallest / len(split), top_value / len(split)))
        factor_of = factor_of * jnp.repeat(draws, extent[position] // blocks).reshape([-1 if axis == position else 1 for axis in range(len(extent))])
    return factor_of


def shared_out(own_key, own, number, rows, count, top, bound, skew):
    order = jax.random.permutation(own_key, count)
    heavy_load, usual = shares(count, rows * top, bound, skew, True), shares(count, rows * top, bound, skew, False)
    places = jnp.arange(count)

    def named(lengths, rotation):
        used = int((lengths > 0).sum())
        fixed = max(1, used // 4)
        moved = fixed + (places - fixed + rotation * (used - fixed)) % max(1, count - fixed)
        return jnp.zeros((count,), jnp.int32).at[order[jnp.where(places < fixed, places, moved)]].set(jnp.asarray(lengths, jnp.int32))

    lengths = jnp.where(number % 4 == 0, named(heavy_load, number // 4), named(usual, number - number // 4 - 1))
    mixed = jax.random.permutation(jax.random.fold_in(own, 3), count)
    source_of, sink = mixed[0:count // 2 * 2:2], mixed[1:count // 2 * 2:2]
    slack = jnp.minimum(lengths[source_of] - 1, bound - lengths[sink]) // 2
    slack = jnp.where((source_of == order[0]) | (sink == order[0]) | (lengths[sink] == 0), 0, jnp.maximum(slack, 0))
    moved = jax.random.randint(jax.random.fold_in(own, 4), (count // 2,), 0, 1 << 20) % (slack + 1)
    lengths = lengths.at[source_of].add(-moved).at[sink].add(moved)
    items = jnp.searchsorted(jnp.cumsum(lengths), jnp.arange(rows * top), side="right").astype(jnp.int32)
    listing = items.reshape(top, rows).T
    listing = listing[jax.random.permutation(jax.random.fold_in(own, 1), rows)]
    rotation = jax.random.randint(jax.random.fold_in(own, 2), (rows, 1), 0, top)
    return jnp.take_along_axis(listing, (jnp.arange(top)[None, :] + rotation) % top, axis=1)


def shares(count, total, limit, lean, full):
    portions = [(1 << 20) // math.isqrt(grade ** lean) + 1 for grade in range(1, count + 1)]
    largest = limit if full else min(limit, max(-(-total // count), total * portions[0] // sum(portions)))
    least = 1 if total - largest >= count - 1 else 0
    counts, rest = [largest] + [least] * (count - 1), total - largest - least * (count - 1)
    while rest > 0:
        free = [i for i in range(1, count) if counts[i] < largest] or [i for i in range(1, count) if counts[i] < limit]
        mass, budget = sum([portions[i] for i in free]), rest
        for i in free:
            addition = min(limit - counts[i], max(1, budget * portions[i] // mass), rest)
            counts[i] = counts[i] + addition
            rest = rest - addition
    return np.array(counts)


def scatter_about(own_key, extent, scale, most, split=(), held_as=jnp.bfloat16):
    loudness = shard_levels(own_key, extent, split, -0.22, 0.18) if split else 1.0
    values = jax.random.normal(own_key, extent, jnp.float32) * scale * loudness
    return jnp.minimum(jnp.maximum(values, -most), most).astype(held_as)


def setup_inputs(seed: int = 0) -> dict:
    splits = jax.random.split(jax.random.key(seed), 7)
    stream = scatter_about(splits[0], (2, PIPE, TOKENS, D), 1.0, 6.0, ((1, 4), (2, 4), (3, 2)))
    expert_ids_keys = jax.random.split(jax.random.fold_in(splits[1], 1), 2 * PIPE * TOKENS // TOK_DEV)
    expert_ids_turns = jax.random.permutation(jax.random.fold_in(splits[1], 3), 2 * PIPE * TOKENS // TOK_DEV)
    expert_ids = jax.vmap(lambda own, number: shared_out(jax.random.fold_in(splits[1], 2), own, number, TOK_DEV, EXPERTS, TOP, CAP, 2))(expert_ids_keys, expert_ids_turns).reshape((2, PIPE, TOKENS, TOP))
    norm_gain = jnp.clip(1.0 + 0.18 * jax.random.normal(splits[2], (PIPE, D), jnp.float32), 0.1, 1.9)
    router = scatter_about(splits[3], (PIPE, D, EXPERTS), D ** -0.5, 0.0625, ((0, 4), (1, 2)), jnp.float32)
    w_up = scatter_about(splits[4], (EXPERTS, D, FF), D ** -0.5, 0.0625, ((0, 4), (1, 2)))
    w_down = scatter_about(splits[5], (EXPERTS, FF, D), FF ** -0.5, 0.1875, ((0, 4), (2, 2)))
    return dict(stream=stream, expert_ids=expert_ids, norm_gain=norm_gain, router=router, w_up=w_up, w_down=w_down)


norm_eps = 1e-06
route_scale = 2.5

def reference(stream, expert_ids, norm_gain, router, w_up, w_down):
    ahead = jnp.roll(stream[0], 1, axis=0)
    behind = jnp.roll(stream[1], -1, axis=0)
    arrived = jnp.stack([ahead, behind]).astype(jnp.float32)
    inverse = lax.rsqrt(lax.optimization_barrier(jnp.mean(arrived * arrived, axis=-1)) + norm_eps)
    normed = arrived * norm_gain[None, :, None, :] * inverse[..., None]
    logits = jnp.einsum('dptc,pce->dpte', normed, router, precision=lax.Precision.HIGHEST)
    picked = jnp.take_along_axis(logits, expert_ids, axis=-1)
    scores = jax.nn.sigmoid(picked)
    gates = route_scale * scores / lax.optimization_barrier(jnp.sum(scores, axis=-1, keepdims=True))
    hidden = normed.astype(jnp.bfloat16)
    groups = expert_ids.reshape(2, PIPE, N_EXPERT, TOK_DEV * TOP)
    onehot = (groups[..., None] == jnp.arange(EXPERTS, dtype=jnp.int32)).astype(jnp.int32)
    earlier = jnp.cumsum(onehot, axis=3) - onehot
    within = lax.optimization_barrier(jnp.sum(earlier * onehot, axis=-1))
    heading = lax.broadcasted_iota(jnp.int32, groups.shape, 0)
    section = lax.broadcasted_iota(jnp.int32, groups.shape, 1)
    member = lax.broadcasted_iota(jnp.int32, groups.shape, 2)
    entry = lax.broadcasted_iota(jnp.int32, groups.shape, 3)
    place = ((section * N_EXPERT + member) * 2 + heading) * CAP + within
    anchor = ((heading * PIPE + section) * N_EXPERT + member) * TOK_DEV + entry // TOP
    length = PIPE * N_EXPERT * 2 * CAP
    owner = jnp.full((EXPERTS, length), 2 * PIPE * TOKENS, jnp.int32).at[groups, place].set(anchor)
    width = hidden.shape[-1]
    table = jnp.concatenate([hidden.reshape(-1, width), jnp.zeros((1, width), jnp.bfloat16)], axis=0)

    def expert_rows(pieces):
        owned, upper, lower = pieces
        inner = jnp.dot(table[owned], upper, preferred_element_type=jnp.float32)
        active = jax.nn.silu(inner).astype(jnp.bfloat16)
        return jnp.dot(active, lower, preferred_element_type=jnp.float32).astype(jnp.bfloat16)
    produced = lax.map(expert_rows, (owner, w_up, w_down))

    def combine(pieces):
        chosen, spots, weights = pieces
        rows = produced[chosen, spots].astype(jnp.float32)
        rows = rows.reshape(N_EXPERT * TOK_DEV, TOP, width)
        return jnp.einsum('tk,tkc->tc', weights, rows)
    mixed = lax.map(combine, (groups.reshape(2 * PIPE, N_EXPERT, TOK_DEV * TOP), place.reshape(2 * PIPE, N_EXPERT, TOK_DEV * TOP), gates.reshape(2 * PIPE, TOKENS, TOP)))
    result = arrived + mixed.reshape(arrived.shape)
    return result.astype(jnp.bfloat16)
```

```python
import functools

import jax
import jax.numpy as jnp
from jax import lax
from jax.experimental import pallas as pl
from jax.experimental.pallas import tpu as pltpu
from jax.sharding import PartitionSpec as P

norm_eps = 1e-06
route_scale = 2.5
MESH = pl.DeviceIdType.MESH


def pieces_of(width, most):
    for count in range(most, 0, -1):
        if width % (count * 128) == 0:
            return count
    return 1


def layer(
    sizes, slots, feat, cols,
    stream, ids_ref, gain_hbm, router_ref, up_hbm, down_hbm, out_ref,
    up, down, arrived, send, recv, rows32, inner, part, parts_in, active, squares, squares_in,
    small, small_in, ret, back, weights, gain_ref,
    load_sem, shift_send, shift_recv, disp_send, disp_recv, ten_send, ten_recv, ret_send, ret_recv,
):
    n_pipe, n_exp, n_ten = sizes
    pipe, expert, tensor = lax.axis_index("pipe"), lax.axis_index("expert"), lax.axis_index("tensor")
    tokens, width = arrived.shape
    half = tokens // 2
    hidden_units = up.shape[1]
    experts = router_ref.shape[0]
    step_f, step_c = width // feat, hidden_units // cols

    def section(by):
        return (lax.rem(pipe + by + n_pipe, n_pipe), expert, tensor)

    def member(by):
        return (pipe, lax.rem(expert + by + n_exp, n_exp), tensor)

    def holder(by):
        return (pipe, expert, lax.rem(tensor + by + n_ten, n_ten))

    barrier = pltpu.get_barrier_semaphore()
    greeted = [section(1), section(-1)]
    greeted += [member(o) for o in range(1, n_exp)] + [holder(o) for o in range(1, n_ten)]
    for who in greeted:
        pl.semaphore_signal(barrier, inc=1, device_id=who, device_id_type=MESH)

    loads = []
    for f in range(feat):
        at = pl.ds(f * step_f, step_f)
        loads.append(pltpu.make_async_copy(up_hbm.at[0, at], up.at[at], load_sem.at[f]))
    loads.append(pltpu.make_async_copy(down_hbm.at[0], down, load_sem.at[feat]))
    gain_load = pltpu.make_async_copy(
        gain_hbm, gain_ref.at[:, pl.ds(0, width)], load_sem.at[feat + 1]
    )
    gain_load.start()
    for load in loads:
        load.start()
    pl.semaphore_wait(barrier, len(greeted))

    shifts = [
        pltpu.make_async_remote_copy(
            src_ref=stream.at[d, 0], dst_ref=arrived.at[pl.ds(d * half, half)],
            send_sem=shift_send.at[d], recv_sem=shift_recv.at[d],
            device_id=section(1 - 2 * d), device_id_type=MESH,
        )
        for d in range(2)
    ]
    for copy in shifts:
        copy.start()

    ids = ids_ref[...]
    total = n_exp * slots
    lane = lax.broadcasted_iota(jnp.int32, (tokens, total), 1)
    block = lane // slots
    lane_expert = lax.rem(block + expert, n_exp)
    takes = jnp.zeros((tokens, total), jnp.float32)
    for k in range(ids.shape[1]):
        takes += jnp.where(ids[:, k : k + 1] == lane_expert, 1.0, 0.0)
    below = lax.broadcasted_iota(jnp.int32, (tokens, tokens), 0) > lax.broadcasted_iota(
        jnp.int32, (tokens, tokens), 1
    )
    rank = jnp.dot(
        jnp.where(below, 1.0, 0.0).astype(jnp.bfloat16),
        takes.astype(jnp.bfloat16),
        preferred_element_type=jnp.float32,
    )
    spot = (lane - block * slots).astype(jnp.float32)
    place = jnp.where((rank == spot) & (takes > 0.0), 1.0, 0.0)
    pick = place.astype(jnp.bfloat16)

    for copy in shifts:
        copy.wait_recv()

    dispatch = {}
    for f in range(feat):
        at = pl.ds(f * step_f, step_f)
        taken = lax.dot_general(
            pick, arrived[:, at], (((0,), (0,)), ((), ())), preferred_element_type=jnp.float32
        ).astype(jnp.float32)
        for o in list(range(1, n_exp)) + [0]:
            rows = taken[o * slots : (o + 1) * slots].astype(jnp.bfloat16)
            if o == 0:
                recv[0, 0:slots, at] = rows
                continue
            send[o, 0:slots, at] = rows
            dispatch[o, f] = pltpu.make_async_remote_copy(
                src_ref=send.at[o, pl.ds(0, slots), at], dst_ref=recv.at[o, pl.ds(0, slots), at],
                send_sem=disp_send.at[o, f], recv_sem=disp_recv.at[o, f],
                device_id=member(o), device_id_type=MESH,
            )
            dispatch[o, f].start()

    gain_load.wait()
    held = arrived[...].astype(jnp.float32)
    small[0] = jnp.broadcast_to(jnp.sum(held * held, axis=1, keepdims=True), (tokens, 128))
    small[1] = jnp.zeros((tokens, 128), jnp.float32)
    small[1, :, 0:experts] = lax.dot_general(
        held * gain_ref[:, 0:width], router_ref[...], (((1,), (1,)), ((), ())),
        preferred_element_type=jnp.float32, precision=lax.Precision.HIGHEST,
    )

    def to_holders(src, dst, sem):
        copies = [
            pltpu.make_async_remote_copy(
                src_ref=src, dst_ref=dst(o), send_sem=ten_send.at[o, sem], recv_sem=ten_recv.at[o, sem],
                device_id=holder(o), device_id_type=MESH,
            )
            for o in range(1, n_ten)
        ]
        for copy in copies:
            copy.start()
        return copies

    small_copies = to_holders(small, lambda o: small_in.at[o], cols)

    square = jnp.zeros((total, 1), jnp.float32)
    for f in range(feat):
        at = pl.ds(f * step_f, step_f)
        gain = gain_ref[:, at]
        for o in range(n_exp):
            if o > 0:
                dispatch[o, f].wait_recv()
            rows32[pl.ds(o * slots, slots), :] = recv[o, 0:slots, at].astype(jnp.float32)
        rows = rows32[...]
        square += jnp.sum(rows * rows, axis=1, keepdims=True)
        if f == feat - 1:
            squares[...] = jnp.broadcast_to(square, (total, 128))
            square_copies = to_holders(squares, lambda o: squares_in.at[o], cols + 1)
        lifted = (rows * gain).astype(jnp.bfloat16)
        loads[f].wait()
        if f < feat - 1:
            found = jnp.dot(lifted, up[at, :], preferred_element_type=jnp.float32)
            if f == 0:
                inner[...] = found
            else:
                inner[...] += found
    exchange = []
    for c in range(cols):
        units = pl.ds(c * step_c, step_c)
        found = jnp.dot(lifted, up[at, units], preferred_element_type=jnp.float32)
        if feat > 1:
            found += inner[:, units]
        inner[:, units] = found
        part[c] = found.astype(jnp.bfloat16)
        exchange.append(to_holders(part.at[c], lambda o, c=c: parts_in.at[o, c], c))

    for copy in small_copies:
        copy.wait_recv()
    sums, logits = small[0], small[1, :, 0:experts]
    for o in range(1, n_ten):
        sums = sums + small_in[o, 0]
        logits = logits + small_in[o, 1, :, 0:experts]
    full = float(width * n_ten)
    logits = logits * lax.rsqrt(sums[:, 0:1] / full + norm_eps)
    which = lax.broadcasted_iota(jnp.int32, logits.shape, 1)
    scores = []
    for k in range(ids.shape[1]):
        picked = jnp.sum(jnp.where(ids[:, k : k + 1] == which, logits, 0.0), axis=1, keepdims=True)
        scores.append(1.0 / (1.0 + jnp.exp(-picked)))
    norm = scores[0]
    for score in scores[1:]:
        norm = norm + score
    gate = jnp.zeros((tokens, total), jnp.float32)
    for k, score in enumerate(scores):
        gate += jnp.where(ids[:, k : k + 1] == lane_expert, route_scale * score / norm, 0.0)
    gate = gate * place
    coarse = gate.astype(jnp.bfloat16)
    weights[0, :, 0:total] = coarse
    weights[1, :, 0:total] = (gate - coarse.astype(jnp.float32)).astype(jnp.bfloat16)

    for copy in square_copies:
        copy.wait_recv()
    total_sq = squares[...]
    for o in range(1, n_ten):
        total_sq = total_sq + squares_in[o]
    inverse = lax.rsqrt(total_sq[:, 0:1] / full + norm_eps)
    for c in range(cols):
        units = pl.ds(c * step_c, step_c)
        for copy in exchange[c]:
            copy.wait_recv()
        value = inner[:, units]
        for o in range(1, n_ten):
            value = value + parts_in[o, c].astype(jnp.float32)
        value = value * inverse
        active[:, units] = (value / (1.0 + jnp.exp(-value))).astype(jnp.bfloat16)

    loads[feat].wait()
    returns = {}
    for f in range(feat):
        at = pl.ds(f * step_f, step_f)
        made = jnp.dot(active[...], down[:, at], preferred_element_type=jnp.float32)
        for o in list(range(1, n_exp)) + [0]:
            rows = made[o * slots : (o + 1) * slots].astype(jnp.bfloat16)
            if o == 0:
                back[0, 0:slots, at] = rows
                continue
            ret[o, 0:slots, at] = rows
            returns[o, f] = pltpu.make_async_remote_copy(
                src_ref=ret.at[o, pl.ds(0, slots), at], dst_ref=back.at[o, pl.ds(0, slots), at],
                send_sem=ret_send.at[o, f], recv_sem=ret_recv.at[o, f],
                device_id=member(-o), device_id_type=MESH,
            )
            returns[o, f].start()

    for f in range(feat):
        at = pl.ds(f * step_f, step_f)
        for o in range(n_exp):
            if o > 0:
                returns[o, f].wait_recv()
            rows32[pl.ds(o * slots, slots), :] = back[o, 0:slots, at].astype(jnp.float32)
        rows = rows32[...].astype(jnp.bfloat16)
        mixed = jnp.dot(weights[0, :, 0:total], rows, preferred_element_type=jnp.float32)
        mixed += jnp.dot(weights[1, :, 0:total], rows, preferred_element_type=jnp.float32)
        out_ref[:, at] = (arrived[:, at].astype(jnp.float32) + mixed).astype(jnp.bfloat16)

    for copies in [shifts, dispatch.values(), small_copies, square_copies, returns.values()] + exchange:
        for copy in copies:
            copy.wait_send()


def relay(
    sizes, pieces,
    stream, ids_ref, gain_hbm, router_hbm, up_hbm, down_hbm, out_hbm,
    up, down, mine, arrived, pool, inner, part, part_in, small, small_in, meta, acc, opp_made,
    ret_send, ret_in, comb_in, res, gain_ref, router_ref,
    load_sem, out_sem, shift_send, shift_recv, disp_send, disp_recv, ten_send, ten_recv,
    meta_send, meta_recv, rets_send, rets_recv, comb_recv,
):
    n_pipe, n_exp, n_ten = sizes
    pipe, expert, tensor = lax.axis_index("pipe"), lax.axis_index("expert"), lax.axis_index("tensor")
    rows, width = arrived.shape[1:]
    hidden_units = up.shape[1]
    experts = router_ref.shape[0]
    step = width // pieces
    bf16, f32 = jnp.bfloat16, jnp.float32

    side = expert // 2
    inside = lax.rem((expert + 1) // 2, 2)
    outside = 1 - inside

    def at_expert(z):
        return (pipe, z, tensor)

    partner = at_expert(expert + 1 - 2 * lax.rem(expert, 2))
    across = [at_expert(2 - side), at_expert(3 - 3 * side)]
    holder = (pipe, expert, 1 - tensor)
    after, before = lax.rem(pipe + 1, n_pipe), lax.rem(pipe + n_pipe - 1, n_pipe)
    sections = [(after, expert, tensor), (before, expert, tensor)]

    barrier = pltpu.get_barrier_semaphore()
    for who in sections + [holder, partner, across[0]]:
        pl.semaphore_signal(barrier, inc=1, device_id=who, device_id_type=MESH)

    @pl.when(inside == 1)
    def _():
        pl.semaphore_signal(barrier, inc=1, device_id=across[1], device_id_type=MESH)

    spans = [pl.ds(f * step, step) for f in range(pieces)]
    mine_load = pltpu.make_async_copy(stream.at[:, 0], mine, load_sem.at[0])
    gain_load = pltpu.make_async_copy(gain_hbm, gain_ref.at[:, pl.ds(0, width)], load_sem.at[1])
    router_load = pltpu.make_async_copy(router_hbm, router_ref, load_sem.at[2])
    up_loads = [
        pltpu.make_async_copy(up_hbm.at[0, at], up.at[at], load_sem.at[3 + f])
        for f, at in enumerate(spans)
    ]
    down_load = pltpu.make_async_copy(down_hbm.at[0], down, load_sem.at[3 + pieces])
    for load in [mine_load, gain_load, router_load] + up_loads + [down_load]:
        load.start()

    def heading(c):
        return lax.rem(pipe + 1 + c, 2)

    lane = lax.broadcasted_iota(jnp.int32, (rows, 128), 1)
    square = (rows, rows)
    eye = jnp.where(
        lax.broadcasted_iota(jnp.int32, square, 0) == lax.broadcasted_iota(jnp.int32, square, 1), 1.0, 0.0
    ).astype(bf16)
    both = ids_ref[...]
    kind = lax.broadcasted_iota(jnp.int32, (128, rows), 0)
    named = []
    for d in range(2):
        marks = jnp.zeros((128, rows), f32)
        for k in range(both.shape[1]):
            marks += jnp.where(both[d, k : k + 1, :] == kind, 1.0, 0.0)
        named.append(
            lax.dot_general(eye, marks.astype(bf16), (((1,), (1,)), ((), ())), preferred_element_type=f32)
        )
    chosen = [jnp.where(heading(c) == 0, named[0], named[1]) for c in range(2)]

    mine_load.wait()
    pl.semaphore_wait(barrier, 5 + inside)

    def remote(src, dst, send, recv, who):
        return pltpu.make_async_remote_copy(
            src_ref=src, dst_ref=dst, send_sem=send, recv_sem=recv, device_id=who, device_id_type=MESH
        )

    started, inner_only, outer_only = [], [], []
    lands = [lax.rem(after + 1, 2), lax.rem(before, 2)]
    shifts = [
        remote(
            mine.at[d], arrived.at[lands[d]], shift_send.at[d], shift_recv.at[lands[d]], sections[d]
        )
        for d in range(2)
    ]
    for copy in shifts:
        copy.start()
        started.append(copy)

    own, mate = pl.ds(0, rows), pl.ds(rows, rows)
    gain_load.wait()
    router_load.wait()

    def take_in(c):
        remote(mine.at[0], arrived.at[c], shift_send.at[0], shift_recv.at[c], sections[0]).wait_recv()
        for at in spans:
            pool[c, 0, 0:rows, at] = (arrived[c, :, at].astype(f32) * gain_ref[:, at]).astype(bf16)
        copies = [
            remote(
                pool.at[c, 0, own, at], pool.at[c, 0, mate, at],
                disp_send.at[0, c, f], disp_recv.at[0, c, f], partner,
            )
            for f, at in enumerate(spans)
        ]
        there = pl.ds(pl.multiple_of(rows * outside, rows), rows)
        copies += [
            remote(
                pool.at[c, 0, own, at], pool.at[c, 1, there, at],
                disp_send.at[1, c, f], disp_recv.at[1 + outside, c, f], across[0],
            )
            for f, at in enumerate(spans)
        ]
        for copy in copies:
            copy.start()
            started.append(copy)
        total = jnp.zeros((rows, 1), f32)
        found = [jnp.zeros((rows, 1), f32) for _ in range(experts)]
        for at in spans:
            held = arrived[c, :, at].astype(f32)
            total += jnp.sum(held * held, axis=1, keepdims=True)
            lifted = held * gain_ref[:, at]
            routes = router_ref[:, at]
            for x in range(experts):
                found[x] += jnp.sum(lifted * routes[x : x + 1], axis=1, keepdims=True)
        tile = jnp.where(lane == experts, total, 0.0)
        for x in range(experts):
            tile = jnp.where(lane == x, found[x], tile)
        small[c] = tile
        copy = remote(
            small.at[c], small_in.at[c], ten_send.at[6 + c], ten_recv.at[6 + c], holder
        )
        copy.start()
        started.append(copy)
        return copy

    full = float(width * n_ten)

    def weigh(c, copy):
        copy.wait_recv()
        tile = small[c] + small_in[c]
        inverse = lax.rsqrt(tile[:, experts : experts + 1] / full + norm_eps)
        scores = 1.0 / (1.0 + jnp.exp(-(tile * inverse)))
        scores = jnp.where(chosen[c] > 0.0, scores, 0.0)
        norm = jnp.sum(scores, axis=1, keepdims=True)
        meta[c, 0, 0:rows] = jnp.where(lane == experts, inverse, route_scale * scores / norm)
        there = pl.ds(pl.multiple_of(rows * outside, rows), rows)
        copies = [
            remote(meta.at[c, 0, own], meta.at[c, 0, mate], meta_send.at[0, c], meta_recv.at[0, c], partner),
            remote(
                meta.at[c, 0, own], meta.at[c, 1, there],
                meta_send.at[1, c], meta_recv.at[1 + outside, c], across[0],
            ),
        ]
        for copy in copies:
            copy.start()
            started.append(copy)

    def forward(c, j):
        spot = pl.ds(j * rows, rows)
        copies = [
            remote(
                pool.at[c, 1, spot, at], pool.at[c, 1, spot, at],
                disp_send.at[2 + j, c, f], disp_recv.at[1 + j, c, f], partner,
            )
            for f, at in enumerate(spans)
        ]

        @pl.when(inside == 1)
        def _():
            for copy in copies:
                copy.wait_recv()
                copy.start()

        inner_only.extend(copies)

    def forward_meta(c, j):
        spot = pl.ds(j * rows, rows)
        copy = remote(
            meta.at[c, 1, spot], meta.at[c, 1, spot],
            meta_send.at[2 + j, c], meta_recv.at[1 + j, c], partner,
        )

        @pl.when(inside == 1)
        def _():
            copy.wait_recv()
            copy.start()

        inner_only.append(copy)

    passes = [(0, 0, 0, 2), (1, 0, 0, 2), (0, 1, 0, 1), (0, 1, 1, 1), (1, 1, 0, 1), (1, 1, 1, 1)]
    loaded = set()
    exchange = {}

    def go_up(p):
        c, g, first, many = passes[p]
        spot = pl.ds(first * rows, many * rows)
        total = None
        for f, at in enumerate(spans):
            if g == 0:
                remote(
                    pool.at[c, 0, own, at], pool.at[c, 0, mate, at],
                    disp_send.at[0, c, f], disp_recv.at[0, c, f], partner,
                ).wait_recv()
            else:
                waits = remote(
                    pool.at[c, 1, spot, at], pool.at[c, 1, spot, at],
                    disp_send.at[2 + first, c, f], disp_recv.at[1 + first, c, f], partner,
                )
                pl.when(outside == 1)(waits.wait_recv)
            if f not in loaded:
                up_loads[f].wait()
                loaded.add(f)
            found = jnp.dot(pool[c, g, spot, at], up[at, :], preferred_element_type=f32)
            if f > 0:
                found += inner[c, g, spot, :]
            inner[c, g, spot, :] = found
        part[c, g, spot, :] = found.astype(bf16)
        exchange[p] = remote(
            part.at[c, g, spot], part_in.at[c, g, spot], ten_send.at[p], ten_recv.at[p], holder
        )
        exchange[p].start()
        started.append(exchange[p])

    def go_down(p):
        c, g, first, many = passes[p]
        spot = pl.ds(first * rows, many * rows)
        if g == 0:
            remote(
                meta.at[c, 0, own], meta.at[c, 0, mate], meta_send.at[0, c], meta_recv.at[0, c], partner
            ).wait_recv()
        else:
            waits = remote(
                meta.at[c, 1, spot], meta.at[c, 1, spot],
                meta_send.at[2 + first, c], meta_recv.at[1 + first, c], partner,
            )
            pl.when(outside == 1)(waits.wait_recv)
        tile = meta[c, g, spot]
        wide = lax.broadcasted_iota(jnp.int32, tile.shape, 1)
        gate = jnp.sum(jnp.where(wide == expert, tile, 0.0), axis=1, keepdims=True)
        inverse = tile[:, experts : experts + 1]
        exchange[p].wait_recv()
        value = (inner[c, g, spot, :] + part_in[c, g, spot, :].astype(f32)) * inverse
        active = (gate * (value / (1.0 + jnp.exp(-value)))).astype(bf16)
        if p == 0:
            down_load.wait()
        for f, at in enumerate(spans):
            made = jnp.dot(active, down[:, at], preferred_element_type=f32)
            if g == 0:
                acc[c, :, at] = arrived[c, :, at].astype(f32) + made[0:rows]
                ret_send[c, 0, :, at] = made[rows:].astype(bf16)
                copy = remote(
                    ret_send.at[c, 0, :, at], ret_in.at[c, 0, :, at],
                    rets_send.at[0, c, f], rets_recv.at[0, c, f], partner,
                )
                copy.start()
                started.append(copy)
                continue
            copy = remote(
                ret_send.at[c, 1 + first, :, at], comb_in.at[c, first, :, at],
                rets_send.at[1 + first, c, f], comb_recv.at[first, c, f], partner,
            )
            outer_only.append(copy)

            @pl.when(outside == 1)
            def _():
                ret_send[c, 1 + first, :, at] = made.astype(bf16)
                copy.start()

            @pl.when(inside == 1)
            def _():
                opp_made[c, first, :, at] = made

    def combine(c, j):
        for f, at in enumerate(spans):
            waits = remote(
                ret_send.at[c, 1 + j, :, at], comb_in.at[c, j, :, at],
                rets_send.at[1 + j, c, f], comb_recv.at[j, c, f], partner,
            )
            copy = remote(
                ret_send.at[c, 1 + j, :, at], ret_in.at[c, 1, :, at],
                rets_send.at[1 + j, c, f], rets_recv.at[1, c, f], across[j],
            )
            inner_only.append(copy)

            @pl.when(inside == 1)
            def _():
                waits.wait_recv()
                ret_send[c, 1 + j, :, at] = (
                    opp_made[c, j, :, at] + comb_in[c, j, :, at].astype(f32)
                ).astype(bf16)
                copy.start()

    outs = []

    def finish(c):
        for f, at in enumerate(spans):
            for k in range(2):
                remote(
                    ret_send.at[c, 0, :, at], ret_in.at[c, k, :, at],
                    rets_send.at[0, c, f], rets_recv.at[k, c, f], partner,
                ).wait_recv()
            total = acc[c, :, at] + ret_in[c, 0, :, at].astype(f32) + ret_in[c, 1, :, at].astype(f32)
            res[c, :, at] = total.astype(bf16)
        copy = pltpu.make_async_copy(res.at[c], out_hbm.at[heading(c)], out_sem.at[c])
        copy.start()
        outs.append(copy)

    near = take_in(0)
    far = take_in(1)
    weigh(0, near)
    forward(0, 0)
    go_up(0)
    weigh(1, far)
    forward(0, 1)
    forward_meta(0, 0)
    forward_meta(0, 1)
    go_up(1)
    forward(1, 0)
    go_down(0)
    go_up(2)
    forward(1, 1)
    forward_meta(1, 0)
    forward_meta(1, 1)
    go_down(1)
    go_up(3)
    go_down(2)
    go_up(4)
    go_down(3)
    go_up(5)
    go_down(4)
    go_down(5)
    combine(0, 0)
    combine(0, 1)
    finish(0)
    combine(1, 0)
    combine(1, 1)
    finish(1)

    for copy in started:
        copy.wait_send()

    @pl.when(inside == 1)
    def _():
        for copy in inner_only:
            copy.wait_send()

    @pl.when(outside == 1)
    def _():
        for copy in outer_only:
            copy.wait_send()

    for copy in outs:
        copy.wait()


def relayed(sizes, stream, expert_ids, norm_gain, router, w_up, w_down):
    n_pipe, n_exp, n_ten = sizes
    rows, width = stream.shape[2:]
    experts = router.shape[2]
    hidden_units = w_up.shape[2]
    pieces = pieces_of(width, 4)
    bf16, f32 = jnp.bfloat16, jnp.float32
    dma = pltpu.SemaphoreType.DMA
    vmem = pl.BlockSpec(memory_space=pltpu.VMEM)
    hbm = pl.BlockSpec(memory_space=pl.ANY)
    result = pl.pallas_call(
        functools.partial(relay, sizes, pieces),
        out_shape=jax.ShapeDtypeStruct((2, rows, width), bf16),
        in_specs=[hbm, vmem, hbm, hbm, hbm, hbm],
        out_specs=hbm,
        scratch_shapes=[
            pltpu.VMEM((width, hidden_units), bf16),
            pltpu.VMEM((hidden_units, width), bf16),
            pltpu.VMEM((2, rows, width), bf16),
            pltpu.VMEM((2, rows, width), bf16),
            pltpu.VMEM((2, 2, 2 * rows, width), bf16),
            pltpu.VMEM((2, 2, 2 * rows, hidden_units), f32),
            pltpu.VMEM((2, 2, 2 * rows, hidden_units), bf16),
            pltpu.VMEM((2, 2, 2 * rows, hidden_units), bf16),
            pltpu.VMEM((2, rows, 128), f32),
            pltpu.VMEM((2, rows, 128), f32),
            pltpu.VMEM((2, 2, 2 * rows, 128), f32),
            pltpu.VMEM((2, rows, width), f32),
            pltpu.VMEM((2, 2, rows, width), f32),
            pltpu.VMEM((2, 3, rows, width), bf16),
            pltpu.VMEM((2, 2, rows, width), bf16),
            pltpu.VMEM((2, 2, rows, width), bf16),
            pltpu.VMEM((2, rows, width), bf16),
            pltpu.VMEM((1, width + 1024), f32),
            pltpu.VMEM((experts, width), f32),
            dma((4 + pieces,)),
            dma((2,)),
            dma((2,)),
            dma((2,)),
            dma((4, 2, pieces)),
            dma((3, 2, pieces)),
            dma((8,)),
            dma((8,)),
            dma((4, 2)),
            dma((3, 2)),
            dma((3, 2, pieces)),
            dma((2, 2, pieces)),
            dma((2, 2, pieces)),
        ],
        compiler_params=pltpu.CompilerParams(
            collective_id=0, has_side_effects=True, vmem_limit_bytes=60 * 1024 * 1024
        ),
    )(stream, expert_ids[:, 0].transpose(0, 2, 1), norm_gain, router[0].T, w_up, w_down)
    return result.reshape(2, 1, rows, width)


def shards(sizes, stream, expert_ids, norm_gain, router, w_up, w_down):
    n_pipe, n_exp, n_ten = sizes
    if n_exp == 4 and n_ten == 2 and n_pipe > 1 and n_pipe % 2 == 0 and router.shape[2] == n_exp:
        return relayed(sizes, stream, expert_ids, norm_gain, router, w_up, w_down)
    tok_rows, width = stream.shape[2:]
    fanout = expert_ids.shape[-1]
    experts = router.shape[2]
    hidden_units = w_up.shape[2]
    tokens = 2 * tok_rows
    capacity = 3 * tok_rows * fanout // (2 * experts)
    slots = -(-2 * capacity // 8) * 8
    total = n_exp * slots
    feat = pieces_of(width, 4)
    cols = pieces_of(hidden_units, 4)
    bf16, f32 = jnp.bfloat16, jnp.float32
    dma = pltpu.SemaphoreType.DMA
    vmem = pl.BlockSpec(memory_space=pltpu.VMEM)
    hbm = pl.BlockSpec(memory_space=pl.ANY)
    result = pl.pallas_call(
        functools.partial(layer, sizes, slots, feat, cols),
        out_shape=jax.ShapeDtypeStruct((tokens, width), bf16),
        in_specs=[hbm, vmem, hbm, vmem, hbm, hbm],
        out_specs=vmem,
        scratch_shapes=[
            pltpu.VMEM((width, hidden_units), bf16),
            pltpu.VMEM((hidden_units, width), bf16),
            pltpu.VMEM((tokens, width), bf16),
            pltpu.VMEM((n_exp, -(-slots // 16) * 16, width), bf16),
            pltpu.VMEM((n_exp, -(-slots // 16) * 16, width), bf16),
            pltpu.VMEM((total, width // feat), f32),
            pltpu.VMEM((total, hidden_units), f32),
            pltpu.VMEM((cols, total, hidden_units // cols), bf16),
            pltpu.VMEM((n_ten, cols, total, hidden_units // cols), bf16),
            pltpu.VMEM((total, hidden_units), bf16),
            pltpu.VMEM((total, 128), f32),
            pltpu.VMEM((n_ten, total, 128), f32),
            pltpu.VMEM((2, tokens, 128), f32),
            pltpu.VMEM((n_ten, 2, tokens, 128), f32),
            pltpu.VMEM((n_exp, -(-slots // 16) * 16, width), bf16),
            pltpu.VMEM((n_exp, -(-slots // 16) * 16, width), bf16),
            pltpu.VMEM((2, tokens, -(-total // 128) * 128), bf16),
            pltpu.VMEM((1, width + 1024), f32),
            dma((feat + 2,)),
            dma((2,)),
            dma((2,)),
            dma((n_exp, feat)),
            dma((n_exp, feat)),
            dma((n_ten, cols + 2)),
            dma((n_ten, cols + 2)),
            dma((n_exp, feat)),
            dma((n_exp, feat)),
        ],
        compiler_params=pltpu.CompilerParams(
            collective_id=0, has_side_effects=True, vmem_limit_bytes=60 * 1024 * 1024
        ),
    )(stream, expert_ids.reshape(tokens, fanout), norm_gain, router[0].T, w_up, w_down)
    return result.reshape(2, 1, tok_rows, width)


def solution(mesh):
    sizes = tuple(mesh.shape[axis] for axis in ("pipe", "expert", "tensor"))
    return jax.shard_map(
        functools.partial(shards, sizes),
        mesh=mesh,
        in_specs=(
            P(None, "pipe", "expert", "tensor"),
            P(None, "pipe", "expert", None),
            P("pipe", "tensor"),
            P("pipe", "tensor", None),
            P("expert", "tensor", None),
            P("expert", None, "tensor"),
        ),
        out_specs=P(None, "pipe", "expert", "tensor"),
        check_vma=False,
    )
```

```python
import functools

import jax
import jax.numpy as jnp
from jax import lax
from jax.experimental import pallas as pl
from jax.experimental.pallas import tpu as pltpu
from jax.sharding import PartitionSpec as P

norm_eps = 1e-06
route_scale = 2.5
MESH = pl.DeviceIdType.MESH


def pieces_of(width, most):
    for count in range(most, 0, -1):
        if width % (count * 128) == 0:
            return count
    return 1


def layer(
    sizes, slots, feat, cols,
    stream, ids_ref, gain_hbm, router_ref, up_hbm, down_hbm, out_ref,
    up, down, arrived, send, recv, rows32, inner, part, parts_in, active, squares, squares_in,
    small, small_in, ret, back, weights, gain_ref,
    load_sem, shift_send, shift_recv, disp_send, disp_recv, ten_send, ten_recv, ret_send, ret_recv,
):
    n_pipe, n_exp, n_ten = sizes
    pipe, expert, tensor = lax.axis_index("pipe"), lax.axis_index("expert"), lax.axis_index("tensor")
    tokens, width = arrived.shape
    half = tokens // 2
    hidden_units = up.shape[1]
    experts = router_ref.shape[0]
    step_f, step_c = width // feat, hidden_units // cols

    def section(by):
        return (lax.rem(pipe + by + n_pipe, n_pipe), expert, tensor)

    def member(by):
        return (pipe, lax.rem(expert + by + n_exp, n_exp), tensor)

    def holder(by):
        return (pipe, expert, lax.rem(tensor + by + n_ten, n_ten))

    barrier = pltpu.get_barrier_semaphore()
    greeted = [section(1), section(-1)]
    greeted += [member(o) for o in range(1, n_exp)] + [holder(o) for o in range(1, n_ten)]
    for who in greeted:
        pl.semaphore_signal(barrier, inc=1, device_id=who, device_id_type=MESH)

    loads = []
    for f in range(feat):
        at = pl.ds(f * step_f, step_f)
        loads.append(pltpu.make_async_copy(up_hbm.at[0, at], up.at[at], load_sem.at[f]))
    loads.append(pltpu.make_async_copy(down_hbm.at[0], down, load_sem.at[feat]))
    gain_load = pltpu.make_async_copy(
        gain_hbm, gain_ref.at[:, pl.ds(0, width)], load_sem.at[feat + 1]
    )
    gain_load.start()
    for load in loads:
        load.start()
    pl.semaphore_wait(barrier, len(greeted))

    shifts = [
        pltpu.make_async_remote_copy(
            src_ref=stream.at[d, 0], dst_ref=arrived.at[pl.ds(d * half, half)],
            send_sem=shift_send.at[d], recv_sem=shift_recv.at[d],
            device_id=section(1 - 2 * d), device_id_type=MESH,
        )
        for d in range(2)
    ]
    for copy in shifts:
        copy.start()

    ids = ids_ref[...]
    total = n_exp * slots
    lane = lax.broadcasted_iota(jnp.int32, (tokens, total), 1)
    block = lane // slots
    lane_expert = lax.rem(block + expert, n_exp)
    takes = jnp.zeros((tokens, total), jnp.float32)
    for k in range(ids.shape[1]):
        takes += jnp.where(ids[:, k : k + 1] == lane_expert, 1.0, 0.0)
    below = lax.broadcasted_iota(jnp.int32, (tokens, tokens), 0) > lax.broadcasted_iota(
        jnp.int32, (tokens, tokens), 1
    )
    rank = jnp.dot(
        jnp.where(below, 1.0, 0.0).astype(jnp.bfloat16),
        takes.astype(jnp.bfloat16),
        preferred_element_type=jnp.float32,
    )
    spot = (lane - block * slots).astype(jnp.float32)
    place = jnp.where((rank == spot) & (takes > 0.0), 1.0, 0.0)
    pick = place.astype(jnp.bfloat16)

    for copy in shifts:
        copy.wait_recv()

    dispatch = {}
    for f in range(feat):
        at = pl.ds(f * step_f, step_f)
        taken = lax.dot_general(
            pick, arrived[:, at], (((0,), (0,)), ((), ())), preferred_element_type=jnp.float32
        ).astype(jnp.float32)
        for o in list(range(1, n_exp)) + [0]:
            rows = taken[o * slots : (o + 1) * slots].astype(jnp.bfloat16)
            if o == 0:
                recv[0, 0:slots, at] = rows
                continue
            send[o, 0:slots, at] = rows
            dispatch[o, f] = pltpu.make_async_remote_copy(
                src_ref=send.at[o, pl.ds(0, slots), at], dst_ref=recv.at[o, pl.ds(0, slots), at],
                send_sem=disp_send.at[o, f], recv_sem=disp_recv.at[o, f],
                device_id=member(o), device_id_type=MESH,
            )
            dispatch[o, f].start()

    gain_load.wait()
    held = arrived[...].astype(jnp.float32)
    small[0] = jnp.broadcast_to(jnp.sum(held * held, axis=1, keepdims=True), (tokens, 128))
    small[1] = jnp.zeros((tokens, 128), jnp.float32)
    small[1, :, 0:experts] = lax.dot_general(
        held * gain_ref[:, 0:width], router_ref[...], (((1,), (1,)), ((), ())),
        preferred_element_type=jnp.float32, precision=lax.Precision.HIGHEST,
    )

    def to_holders(src, dst, sem):
        copies = [
            pltpu.make_async_remote_copy(
                src_ref=src, dst_ref=dst(o), send_sem=ten_send.at[o, sem], recv_sem=ten_recv.at[o, sem],
                device_id=holder(o), device_id_type=MESH,
            )
            for o in range(1, n_ten)
        ]
        for copy in copies:
            copy.start()
        return copies

    small_copies = to_holders(small, lambda o: small_in.at[o], cols)

    square = jnp.zeros((total, 1), jnp.float32)
    for f in range(feat):
        at = pl.ds(f * step_f, step_f)
        gain = gain_ref[:, at]
        for o in range(n_exp):
            if o > 0:
                dispatch[o, f].wait_recv()
            rows32[pl.ds(o * slots, slots), :] = recv[o, 0:slots, at].astype(jnp.float32)
        rows = rows32[...]
        square += jnp.sum(rows * rows, axis=1, keepdims=True)
        if f == feat - 1:
            squares[...] = jnp.broadcast_to(square, (total, 128))
            square_copies = to_holders(squares, lambda o: squares_in.at[o], cols + 1)
        lifted = (rows * gain).astype(jnp.bfloat16)
        loads[f].wait()
        if f < feat - 1:
            found = jnp.dot(lifted, up[at, :], preferred_element_type=jnp.float32)
            if f == 0:
                inner[...] = found
            else:
                inner[...] += found
    exchange = []
    for c in range(cols):
        units = pl.ds(c * step_c, step_c)
        found = jnp.dot(lifted, up[at, units], preferred_element_type=jnp.float32)
        if feat > 1:
            found += inner[:, units]
        inner[:, units] = found
        part[c] = found.astype(jnp.bfloat16)
        exchange.append(to_holders(part.at[c], lambda o, c=c: parts_in.at[o, c], c))

    for copy in small_copies:
        copy.wait_recv()
    sums, logits = small[0], small[1, :, 0:experts]
    for o in range(1, n_ten):
        sums = sums + small_in[o, 0]
        logits = logits + small_in[o, 1, :, 0:experts]
    full = float(width * n_ten)
    logits = logits * lax.rsqrt(sums[:, 0:1] / full + norm_eps)
    which = lax.broadcasted_iota(jnp.int32, logits.shape, 1)
    scores = []
    for k in range(ids.shape[1]):
        picked = jnp.sum(jnp.where(ids[:, k : k + 1] == which, logits, 0.0), axis=1, keepdims=True)
        scores.append(1.0 / (1.0 + jnp.exp(-picked)))
    norm = scores[0]
    for score in scores[1:]:
        norm = norm + score
    gate = jnp.zeros((tokens, total), jnp.float32)
    for k, score in enumerate(scores):
        gate += jnp.where(ids[:, k : k + 1] == lane_expert, route_scale * score / norm, 0.0)
    gate = gate * place
    coarse = gate.astype(jnp.bfloat16)
    weights[0, :, 0:total] = coarse
    weights[1, :, 0:total] = (gate - coarse.astype(jnp.float32)).astype(jnp.bfloat16)

    for copy in square_copies:
        copy.wait_recv()
    total_sq = squares[...]
    for o in range(1, n_ten):
        total_sq = total_sq + squares_in[o]
    inverse = lax.rsqrt(total_sq[:, 0:1] / full + norm_eps)
    for c in range(cols):
        units = pl.ds(c * step_c, step_c)
        for copy in exchange[c]:
            copy.wait_recv()
        value = inner[:, units]
        for o in range(1, n_ten):
            value = value + parts_in[o, c].astype(jnp.float32)
        value = value * inverse
        active[:, units] = (value / (1.0 + jnp.exp(-value))).astype(jnp.bfloat16)

    loads[feat].wait()
    returns = {}
    for f in range(feat):
        at = pl.ds(f * step_f, step_f)
        made = jnp.dot(active[...], down[:, at], preferred_element_type=jnp.float32)
        for o in list(range(1, n_exp)) + [0]:
            rows = made[o * slots : (o + 1) * slots].astype(jnp.bfloat16)
            if o == 0:
                back[0, 0:slots, at] = rows
                continue
            ret[o, 0:slots, at] = rows
            returns[o, f] = pltpu.make_async_remote_copy(
                src_ref=ret.at[o, pl.ds(0, slots), at], dst_ref=back.at[o, pl.ds(0, slots), at],
                send_sem=ret_send.at[o, f], recv_sem=ret_recv.at[o, f],
                device_id=member(-o), device_id_type=MESH,
            )
            returns[o, f].start()

    for f in range(feat):
        at = pl.ds(f * step_f, step_f)
        for o in range(n_exp):
            if o > 0:
                returns[o, f].wait_recv()
            rows32[pl.ds(o * slots, slots), :] = back[o, 0:slots, at].astype(jnp.float32)
        rows = rows32[...].astype(jnp.bfloat16)
        mixed = jnp.dot(weights[0, :, 0:total], rows, preferred_element_type=jnp.float32)
        mixed += jnp.dot(weights[1, :, 0:total], rows, preferred_element_type=jnp.float32)
        out_ref[:, at] = (arrived[:, at].astype(jnp.float32) + mixed).astype(jnp.bfloat16)

    for copies in [shifts, dispatch.values(), small_copies, square_copies, returns.values()] + exchange:
        for copy in copies:
            copy.wait_send()


def relay(
    sizes, cap,
    stream, ids_hbm, gain_hbm, router_hbm, up_hbm, down_hbm, out_ref,
    ids_ref, up, down, mine, arrived, pool, inner, part, part_in, active, small, small_in, meta, acc, opp_made,
    lhs, spare, pack_out, pack_in, ret_send, ret_in, gain_ref, router_ref,
    load_sem, shift_send, shift_recv, disp_send, disp_recv, ten_send, ten_recv,
    meta_send, meta_recv, rets_send, rets_recv, pack_send, pack_recv,
):
    n_pipe, n_exp, n_ten = sizes
    pipe, expert, tensor = lax.axis_index("pipe"), lax.axis_index("expert"), lax.axis_index("tensor")
    rows, width = arrived.shape[1:]
    experts = router_ref.shape[0]
    bf16, f32 = jnp.bfloat16, jnp.float32
    half = width // 2
    first_part = -(-half // 512) * 256
    subs = [(0, first_part), (first_part, half - first_part)]
    spans = [pl.ds(h * half + at, wide) for h in range(2) for at, wide in subs]
    base = experts + 1
    mate_id = expert + 1 - 2 * lax.rem(expert, 2)

    side = expert // 2
    inside = lax.rem((expert + 1) // 2, 2)
    partner = (pipe, expert + 1 - 2 * lax.rem(expert, 2), tensor)
    across, beyond = (pipe, 2 - side, tensor), (pipe, 3 - 3 * side, tensor)
    holder = (pipe, expert, 1 - tensor)
    after, before = lax.rem(pipe + 1, n_pipe), lax.rem(pipe + n_pipe - 1, n_pipe)
    sections = [(after, expert, tensor), (before, expert, tensor)]

    barrier = pltpu.get_barrier_semaphore()
    for who in sections + [holder, partner]:
        pl.semaphore_signal(barrier, inc=1, device_id=who, device_id_type=MESH)

    @pl.when(inside == 1)
    def _():
        pl.semaphore_signal(barrier, inc=1, device_id=across, device_id_type=MESH)

    mine_load = pltpu.make_async_copy(stream.at[:, 0], mine, load_sem.at[0])
    gain_load = pltpu.make_async_copy(gain_hbm, gain_ref.at[:, pl.ds(0, width)], load_sem.at[1])
    router_load = pltpu.make_async_copy(router_hbm, router_ref, load_sem.at[2])
    down_load = pltpu.make_async_copy(down_hbm.at[0], down, load_sem.at[3])
    ids_load = pltpu.make_async_copy(ids_hbm, ids_ref, load_sem.at[4])
    up_loads = [
        pltpu.make_async_copy(up_hbm.at[0, at], up.at[at], load_sem.at[5 + f])
        for f, at in enumerate(spans)
    ]
    for load in [mine_load, ids_load, gain_load, router_load] + up_loads + [down_load]:
        load.start()

    def heading(c):
        return lax.rem(pipe + 1 + c, 2)

    mine_load.wait()
    pl.semaphore_wait(barrier, 4 + inside)

    def remote(src, dst, send, recv, who):
        return pltpu.make_async_remote_copy(
            src_ref=src, dst_ref=dst, send_sem=send, recv_sem=recv, device_id=who, device_id_type=MESH
        )

    lands = [lax.rem(after + 1, 2), lax.rem(before, 2)]
    shifts = [
        remote(
            mine.at[d], arrived.at[lands[d]], shift_send.at[d], shift_recv.at[lands[d]], sections[d]
        )
        for d in range(2)
    ]
    for copy in shifts:
        copy.start()

    own, mate = pl.ds(0, rows), pl.ds(rows, rows)
    full = float(width * n_ten)
    gain_load.wait()
    router_load.wait()

    lane = lax.broadcasted_iota(jnp.int32, (rows, 128), 1)
    square = (rows, rows)
    eye = jnp.where(
        lax.broadcasted_iota(jnp.int32, square, 0) == lax.broadcasted_iota(jnp.int32, square, 1), 1.0, 0.0
    ).astype(bf16)
    ids_load.wait()
    both = ids_ref[...]
    kind = lax.broadcasted_iota(jnp.int32, (128, rows), 0)
    named = []
    for d in range(2):
        marks = jnp.zeros((128, rows), f32)
        for k in range(both.shape[1]):
            named_id = both[d, k : k + 1, :]
            marks += jnp.where((named_id == kind) | (named_id + base == kind), 1.0, 0.0)
        named.append(
            lax.dot_general(eye, marks.astype(bf16), (((1,), (1,)), ((), ())), preferred_element_type=f32)
        )
    chosen = [jnp.where(heading(c) == 0, named[0], named[1]) for c in range(2)]
    earlier = jnp.where(
        lax.broadcasted_iota(jnp.int32, square, 0) > lax.broadcasted_iota(jnp.int32, square, 1), 1.0, 0.0
    ).astype(bf16)
    slots = [
        jnp.where(mark > 0.0, jnp.dot(earlier, mark.astype(bf16), preferred_element_type=f32), -1.0)
        for mark in chosen
    ]
    slot_id = lax.broadcasted_iota(jnp.int32, square, 1)

    def picks(tile, who):
        wide = lax.broadcasted_iota(jnp.int32, tile.shape, 1)
        slot = jnp.sum(jnp.where(wide == base + who, tile, 0.0), axis=1, keepdims=True)
        low = slot == slot_id.astype(f32)
        high = slot == (slot_id - 4).astype(f32)
        left = jnp.where(low & (slot_id < cap), 1.0, 0.0)
        right = jnp.where((low & (slot_id < 8)) | (high & (slot_id >= 12)), 1.0, 0.0)
        return left.astype(bf16), right.astype(bf16)

    def perform(within):
        started, loaded, exchange = list(shifts), set(), {}

        def go(copy):
            copy.start()
            started.append(copy)

        def rows_to(c, f, src, dst, send, recv, who):
            return remote(
                pool.at[c, *src, spans[f]], pool.at[c, *dst, spans[f]],
                disp_send.at[send, c, f], disp_recv.at[recv, c, f], who,
            )

        def tile_to(c, src, dst, send, recv, who):
            return remote(meta.at[c, *src], meta.at[c, *dst], meta_send.at[send, c], meta_recv.at[recv, c], who)

        def spot(j):
            return pl.ds(j * rows, rows)

        def to_mate(c, f):
            return rows_to(c, f, (0, own), (0, mate), 0, 0, partner)

        def to_other(c, f, j):
            return rows_to(c, f, (0, spot(j)), (1, spot(j)), 1 + j, 1 + j, across)

        def relayed_rows(c, f, j):
            return rows_to(c, f, (1, spot(j)), (1, spot(j)), 3 + j, 1 + j, partner)

        def tile_mate(c):
            return tile_to(c, (0, own), (0, mate), 0, 0, partner)

        def tile_other(c, j):
            return tile_to(c, (0, spot(j)), (1, spot(j)), 1 + j, 1 + j, across)

        def relayed_tile(c, j):
            return tile_to(c, (1, spot(j)), (1, spot(j)), 3 + j, 1 + j, partner)

        def take_in(c):
            remote(mine.at[0], arrived.at[c], shift_send.at[0], shift_recv.at[c], sections[0]).wait_recv()
            for f, at in enumerate(spans):
                pool[c, 0, 0:rows, at] = (arrived[c, :, at].astype(f32) * gain_ref[:, at]).astype(bf16)
            for f in range(len(spans)):
                go(to_mate(c, f))
                if within and c == 0:
                    go(to_other(c, f, 0))
            total = jnp.zeros((rows, 1), f32)
            found = [jnp.zeros((rows, 1), f32) for _ in range(experts)]
            for at in spans:
                held = arrived[c, :, at].astype(f32)
                total += jnp.sum(held * held, axis=1, keepdims=True)
                lifted = held * gain_ref[:, at]
                routes = router_ref[:, at]
                for x in range(experts):
                    found[x] += jnp.sum(lifted * routes[x : x + 1], axis=1, keepdims=True)
            tile = jnp.where(lane == experts, total, 0.0)
            for x in range(experts):
                tile = jnp.where(lane == x, found[x], tile)
            small[c] = tile
            copy = remote(small.at[c], small_in.at[c], ten_send.at[6 + c], ten_recv.at[6 + c], holder)
            go(copy)
            return copy

        def weigh(c, copy):
            copy.wait_recv()
            tile = small[c] + small_in[c]
            inverse = lax.rsqrt(tile[:, experts : experts + 1] / full + norm_eps)
            scores = 1.0 / (1.0 + jnp.exp(-(tile * inverse)))
            scores = jnp.where((chosen[c] > 0.0) & (lane < experts), scores, 0.0)
            norm = jnp.sum(scores, axis=1, keepdims=True)
            tile = jnp.where(lane == experts, inverse, route_scale * scores / norm)
            meta[c, 0, 0:rows] = jnp.where(lane < base, tile, slots[c])
            go(tile_mate(c))
            if within:
                go(tile_other(c, 0))

        def send_across(c):
            for f in range(len(spans)):
                go(to_other(c, f, 0))

        def relay_mate(c):
            for f in range(len(spans)):
                to_mate(c, f).wait_recv()
                go(to_other(c, f, 1))

        def relay_mate_tile(c):
            tile_mate(c).wait_recv()
            go(tile_other(c, 1))

        def relay_rows(c, j):
            for f in range(len(spans)):
                copy = relayed_rows(c, f, j)
                copy.wait_recv()
                go(copy)

        def relay_tile(c, j):
            copy = relayed_tile(c, j)
            copy.wait_recv()
            go(copy)

        def go_up(p, ready=None):
            c, g, first, many = passes[p]
            band = pl.ds(first * rows, many * rows)
            if "up" not in loaded:
                for load in up_loads:
                    load.wait()
                loaded.add("up")
            if ready is not None:
                heard(ready)
            if within:
                found = jnp.dot(pool[c, g, band, :], up[...], preferred_element_type=f32)
            else:
                bounds = [0, width - half, width] if g == 0 else [0, width]
                for low, high in zip(bounds, bounds[1:]):
                    for f in range(2 * low // half, 2 * high // half):
                        (to_mate(c, f) if g == 0 else relayed_rows(c, f, first)).wait_recv()
                    more = jnp.dot(
                        pool[c, g, band, low:high], up[low:high, :], preferred_element_type=f32
                    )
                    found = more if low == 0 else found + more
            if ready is not None:
                activate(ready)
            inner[c, g, band, :] = found
            part[c, g, band, :] = found.astype(bf16)
            exchange[p] = remote(
                part.at[c, g, band], part_in.at[c, g, band], ten_send.at[p], ten_recv.at[p], holder
            )
            go(exchange[p])

        def heard(p):
            c, g, first, many = passes[p]
            if not within:
                (tile_mate(c) if g == 0 else relayed_tile(c, first)).wait_recv()
            exchange[p].wait_recv()
            loaded.add(p)

        def activate(p):
            c, g, first, many = passes[p]
            band = pl.ds(first * rows, many * rows)
            tile = meta[c, g, band]
            wide = lax.broadcasted_iota(jnp.int32, tile.shape, 1)
            gate = jnp.sum(jnp.where(wide == expert, tile, 0.0), axis=1, keepdims=True)
            inverse = tile[:, experts : experts + 1]
            value = (inner[c, g, band, :] + part_in[c, g, band, :].astype(f32)) * inverse
            value = (gate * (value / (1.0 + jnp.exp(-value)))).astype(bf16)
            if within:
                active[c, g, band, :] = value
                return
            k = 0 if g == 0 else 1 + first
            for h, pick in enumerate(picks(tile[-rows:], expert)):
                if g == 0:
                    lhs[c, k, h, rows : 2 * rows, :] = value[0:rows]
                lhs[c, k, h, 0:rows, :] = lax.dot_general(
                    pick, value[-rows:], (((0,), (0,)), ((), ())), preferred_element_type=f32
                ).astype(bf16)

        def packed(c, k, b):
            return remote(
                pack_out.at[c, k, b], pack_in.at[c, k, b], pack_send.at[k, c, b], pack_recv.at[k, c, b], partner
            )

        def go_down(p):
            c, g, first, many = passes[p]
            band = pl.ds(first * rows, many * rows)
            if p not in loaded:
                heard(p)
                activate(p)
            if "down" not in loaded:
                down_load.wait()
                loaded.add("down")
            k = 0 if g == 0 else 1 + first

            def deliver(f, made):
                at = spans[f]
                h, (low, wide) = f // 2, subs[f % 2]
                if within and g == 0:
                    acc[c, :, at] = arrived[c, :, at].astype(f32) + made[0:rows]
                    ret_send[c, 0, :, at] = made[rows:].astype(bf16)
                    go(back_to_mate(c, f))
                elif within:
                    for j in range(2):
                        opp_made[c, j, :, at] = made[j * rows : (j + 1) * rows]
                else:
                    if g == 0:
                        acc[c, :, at] = arrived[c, :, at].astype(f32) + made[rows:]
                    local = pl.ds(low, wide)
                    pack_out[c, k, h, :, local] = made[0:8].astype(bf16)
                    if h == 0:
                        spare[c, k, :, local] = made[8:16]
                    else:
                        pack_out[c, k, 2, :, local] = (spare[c, k, :, local] + made[8:16]).astype(bf16)
                    if f == 1:
                        go(packed(c, k, 0))
                    if f == 3:
                        go(packed(c, k, 2))
                        go(packed(c, k, 1))

            last = None
            for f, at in enumerate(spans):
                left = active[c, g, band, :] if within else lhs[c, k, f // 2, 0 : many * rows, :]
                made = jnp.dot(left, down[:, at], preferred_element_type=f32)
                if last is not None:
                    deliver(f - 1, last)
                last = made
            deliver(len(spans) - 1, last)

        def spread(c, k, f, pick):
            h, (low, wide) = f // 2, subs[f % 2]
            local = pl.ds(low, wide)
            if f == 0:
                packed(c, k, 0).wait_recv()
                packed(c, k, 2).wait_recv()
            if f == 2:
                packed(c, k, 1).wait_recv()
            got = jnp.concatenate(
                [pack_in[c, k, h, :, local].astype(f32), pack_in[c, k, 2, :, local].astype(f32)], axis=0
            ).astype(bf16)
            return jnp.dot(pick[h], got, preferred_element_type=f32)

        def absorb(c):
            pick = picks(meta[c, 0, 0:rows], mate_id)
            for f, at in enumerate(spans):
                acc[c, :, at] += spread(c, 0, f, pick)

        def back_to_mate(c, f):
            at = spans[f]
            return remote(
                ret_send.at[c, 0, :, at], ret_in.at[c, 0, :, at],
                rets_send.at[0, c, f], rets_recv.at[0, c, f], partner,
            )

        def sum_home(c, f, j):
            at = spans[f]
            return remote(
                ret_send.at[c, 1 + j, :, at], ret_in.at[c, 1, :, at],
                rets_send.at[1 + j, c, f], rets_recv.at[1, c, f], beyond if j else across,
            )

        def combine(c, j):
            pick = picks(meta[c, 1, spot(j)], mate_id)
            for f, at in enumerate(spans):
                ret_send[c, 1 + j, :, at] = (
                    opp_made[c, j, :, at] + spread(c, 1 + j, f, pick)
                ).astype(bf16)
                go(sum_home(c, f, j))

        def finish(c):
            for f, at in enumerate(spans):
                total = acc[c, :, at]
                if not within:
                    back_to_mate(c, f).wait_recv()
                    total += ret_in[c, 0, :, at].astype(f32)
                sum_home(c, f, 0).wait_recv()
                total += ret_in[c, 1, :, at].astype(f32)
                out_ref[heading(c), :, at] = total.astype(bf16)

        near = take_in(0)
        far = take_in(1)
        if within:
            passes = [(0, 0, 0, 2), (0, 1, 0, 2), (1, 0, 0, 2), (1, 1, 0, 2)]
            weigh(0, near)
            relay_rows(0, 0)
            relay_mate(0)
            relay_mate(1)
            relay_mate_tile(0)
            send_across(1)
            weigh(1, far)
            go_up(0)
            relay_rows(0, 1)
            relay_tile(0, 0)
            relay_mate_tile(1)
            go_up(2)
            relay_rows(1, 1)
            relay_tile(0, 1)
            go_up(1, 0)
            relay_tile(1, 1)
            relay_rows(1, 0)
            go_up(3)
            go_down(0)
            relay_tile(1, 0)
            go_down(2)
            go_down(1)
            go_down(3)
            absorb(0)
            absorb(1)
            combine(0, 0)
            combine(0, 1)
            combine(1, 1)
            combine(1, 0)
        else:
            passes = [(0, 0, 0, 2), (1, 0, 0, 2), (0, 1, 0, 1), (0, 1, 1, 1), (1, 1, 1, 1), (1, 1, 0, 1)]
            weigh(0, near)
            go_up(0)
            weigh(1, far)
            go_up(1)
            go_down(0)
            go_up(2)
            go_down(1)
            go_up(3)
            go_up(4, 2)
            go_down(2)
            go_down(3)
            go_up(5)
            go_down(4)
            go_down(5)
        finish(0)
        finish(1)
        for copy in started:
            copy.wait_send()

    @pl.when(inside == 1)
    def _():
        perform(True)

    @pl.when(inside == 0)
    def _():
        perform(False)


def relayed(sizes, stream, expert_ids, norm_gain, router, w_up, w_down):
    n_pipe, n_exp, n_ten = sizes
    rows, width = stream.shape[2:]
    experts, fanout = router.shape[2], expert_ids.shape[3]
    hidden_units = w_up.shape[2]
    cap = 3 * rows * fanout // (2 * experts)
    pieces = 4
    bf16, f32 = jnp.bfloat16, jnp.float32
    dma = pltpu.SemaphoreType.DMA
    vmem = pl.BlockSpec(memory_space=pltpu.VMEM)
    hbm = pl.BlockSpec(memory_space=pl.ANY)
    result = pl.pallas_call(
        functools.partial(relay, sizes, cap),
        out_shape=pltpu.VMEM((2, rows, width), bf16),
        in_specs=[hbm] * 6,
        out_specs=vmem,
        scratch_shapes=[
            pltpu.VMEM((2, fanout, rows), jnp.int32),
            pltpu.VMEM((width, hidden_units), bf16),
            pltpu.VMEM((hidden_units, width), bf16),
            pltpu.VMEM((2, rows, width), bf16),
            pltpu.VMEM((2, rows, width), bf16),
            pltpu.VMEM((2, 2, 2 * rows, width), bf16),
            pltpu.VMEM((2, 2, 2 * rows, hidden_units), f32),
            pltpu.VMEM((2, 2, 2 * rows, hidden_units), bf16),
            pltpu.VMEM((2, 2, 2 * rows, hidden_units), bf16),
            pltpu.VMEM((2, 2, 2 * rows, hidden_units), bf16),
            pltpu.VMEM((2, rows, 128), f32),
            pltpu.VMEM((2, rows, 128), f32),
            pltpu.VMEM((2, 2, 2 * rows, 128), f32),
            pltpu.VMEM((2, rows, width), f32),
            pltpu.VMEM((2, 2, rows, width), f32),
            pltpu.VMEM((2, 3, 2, 2 * rows, hidden_units), bf16),
            pltpu.VMEM((2, 3, 8, width // 2), f32),
            pltpu.VMEM((2, 3, 3, 8, width // 2), bf16),
            pltpu.VMEM((2, 3, 3, 8, width // 2), bf16),
            pltpu.VMEM((2, 3, rows, width), bf16),
            pltpu.VMEM((2, 2, rows, width), bf16),
            pltpu.VMEM((1, width + 1024), f32),
            pltpu.VMEM((experts, width), f32),
            dma((5 + pieces,)),
            dma((2,)),
            dma((2,)),
            dma((5, 2, pieces)),
            dma((3, 2, pieces)),
            dma((8,)),
            dma((8,)),
            dma((5, 2)),
            dma((3, 2)),
            dma((3, 2, pieces)),
            dma((2, 2, pieces)),
            dma((3, 2, 3)),
            dma((3, 2, 3)),
        ],
        compiler_params=pltpu.CompilerParams(
            collective_id=0, has_side_effects=True, vmem_limit_bytes=67043328 - 4 * rows * width - 16384
        ),
    )(stream, expert_ids[:, 0].transpose(0, 2, 1), norm_gain, router[0].T, w_up, w_down)
    return result.reshape(2, 1, rows, width)


def shards(sizes, stream, expert_ids, norm_gain, router, w_up, w_down):
    n_pipe, n_exp, n_ten = sizes
    if n_exp == 4 and n_ten == 2 and n_pipe > 1 and n_pipe % 2 == 0 and router.shape[2] == n_exp:
        return relayed(sizes, stream, expert_ids, norm_gain, router, w_up, w_down)
    tok_rows, width = stream.shape[2:]
    fanout = expert_ids.shape[-1]
    experts = router.shape[2]
    hidden_units = w_up.shape[2]
    tokens = 2 * tok_rows
    capacity = 3 * tok_rows * fanout // (2 * experts)
    slots = -(-2 * capacity // 8) * 8
    total = n_exp * slots
    feat = pieces_of(width, 4)
    cols = pieces_of(hidden_units, 4)
    bf16, f32 = jnp.bfloat16, jnp.float32
    dma = pltpu.SemaphoreType.DMA
    vmem = pl.BlockSpec(memory_space=pltpu.VMEM)
    hbm = pl.BlockSpec(memory_space=pl.ANY)
    result = pl.pallas_call(
        functools.partial(layer, sizes, slots, feat, cols),
        out_shape=jax.ShapeDtypeStruct((tokens, width), bf16),
        in_specs=[hbm, vmem, hbm, vmem, hbm, hbm],
        out_specs=vmem,
        scratch_shapes=[
            pltpu.VMEM((width, hidden_units), bf16),
            pltpu.VMEM((hidden_units, width), bf16),
            pltpu.VMEM((tokens, width), bf16),
            pltpu.VMEM((n_exp, -(-slots // 16) * 16, width), bf16),
            pltpu.VMEM((n_exp, -(-slots // 16) * 16, width), bf16),
            pltpu.VMEM((total, width // feat), f32),
            pltpu.VMEM((total, hidden_units), f32),
            pltpu.VMEM((cols, total, hidden_units // cols), bf16),
            pltpu.VMEM((n_ten, cols, total, hidden_units // cols), bf16),
            pltpu.VMEM((total, hidden_units), bf16),
            pltpu.VMEM((total, 128), f32),
            pltpu.VMEM((n_ten, total, 128), f32),
            pltpu.VMEM((2, tokens, 128), f32),
            pltpu.VMEM((n_ten, 2, tokens, 128), f32),
            pltpu.VMEM((n_exp, -(-slots // 16) * 16, width), bf16),
            pltpu.VMEM((n_exp, -(-slots // 16) * 16, width), bf16),
            pltpu.VMEM((2, tokens, -(-total // 128) * 128), bf16),
            pltpu.VMEM((1, width + 1024), f32),
            dma((feat + 2,)),
            dma((2,)),
            dma((2,)),
            dma((n_exp, feat)),
            dma((n_exp, feat)),
            dma((n_ten, cols + 2)),
            dma((n_ten, cols + 2)),
            dma((n_exp, feat)),
            dma((n_exp, feat)),
        ],
        compiler_params=pltpu.CompilerParams(
            collective_id=0, has_side_effects=True, vmem_limit_bytes=60 * 1024 * 1024
        ),
    )(stream, expert_ids.reshape(tokens, fanout), norm_gain, router[0].T, w_up, w_down)
    return result.reshape(2, 1, tok_rows, width)


def solution(mesh):
    sizes = tuple(mesh.shape[axis] for axis in ("pipe", "expert", "tensor"))
    return jax.shard_map(
        functools.partial(shards, sizes),
        mesh=mesh,
        in_specs=(
            P(None, "pipe", "expert", "tensor"),
            P(None, "pipe", "expert", None),
            P("pipe", "tensor"),
            P("pipe", "tensor", None),
            P("expert", "tensor", None),
            P("expert", None, "tensor"),
        ),
        out_specs=P(None, "pipe", "expert", "tensor"),
        check_vma=False,
    )
```

```python
import functools

import jax
import jax.numpy as jnp
from jax import lax
from jax.experimental import pallas as pl
from jax.experimental.pallas import tpu as pltpu
from jax.sharding import PartitionSpec as P

norm_eps = 1e-06
route_scale = 2.5
MESH = pl.DeviceIdType.MESH


def pieces_of(width, most):
    for count in range(most, 0, -1):
        if width % (count * 128) == 0:
            return count
    return 1


def layer(
    sizes, slots, feat, cols,
    stream, ids_ref, gain_hbm, router_ref, up_hbm, down_hbm, out_ref,
    up, down, arrived, send, recv, rows32, inner, part, parts_in, active, squares, squares_in,
    small, small_in, ret, back, weights, gain_ref,
    load_sem, shift_send, shift_recv, disp_send, disp_recv, ten_send, ten_recv, ret_send, ret_recv,
):
    n_pipe, n_exp, n_ten = sizes
    pipe, expert, tensor = lax.axis_index("pipe"), lax.axis_index("expert"), lax.axis_index("tensor")
    tokens, width = arrived.shape
    half = tokens // 2
    hidden_units = up.shape[1]
    experts = router_ref.shape[0]
    step_f, step_c = width // feat, hidden_units // cols

    def section(by):
        return (lax.rem(pipe + by + n_pipe, n_pipe), expert, tensor)

    def member(by):
        return (pipe, lax.rem(expert + by + n_exp, n_exp), tensor)

    def holder(by):
        return (pipe, expert, lax.rem(tensor + by + n_ten, n_ten))

    barrier = pltpu.get_barrier_semaphore()
    greeted = [section(1), section(-1)]
    greeted += [member(o) for o in range(1, n_exp)] + [holder(o) for o in range(1, n_ten)]
    for who in greeted:
        pl.semaphore_signal(barrier, inc=1, device_id=who, device_id_type=MESH)

    loads = []
    for f in range(feat):
        at = pl.ds(f * step_f, step_f)
        loads.append(pltpu.make_async_copy(up_hbm.at[0, at], up.at[at], load_sem.at[f]))
    loads.append(pltpu.make_async_copy(down_hbm.at[0], down, load_sem.at[feat]))
    gain_load = pltpu.make_async_copy(
        gain_hbm, gain_ref.at[:, pl.ds(0, width)], load_sem.at[feat + 1]
    )
    gain_load.start()
    for load in loads:
        load.start()
    pl.semaphore_wait(barrier, len(greeted))

    shifts = [
        pltpu.make_async_remote_copy(
            src_ref=stream.at[d, 0], dst_ref=arrived.at[pl.ds(d * half, half)],
            send_sem=shift_send.at[d], recv_sem=shift_recv.at[d],
            device_id=section(1 - 2 * d), device_id_type=MESH,
        )
        for d in range(2)
    ]
    for copy in shifts:
        copy.start()

    ids = ids_ref[...]
    total = n_exp * slots
    lane = lax.broadcasted_iota(jnp.int32, (tokens, total), 1)
    block = lane // slots
    lane_expert = lax.rem(block + expert, n_exp)
    takes = jnp.zeros((tokens, total), jnp.float32)
    for k in range(ids.shape[1]):
        takes += jnp.where(ids[:, k : k + 1] == lane_expert, 1.0, 0.0)
    below = lax.broadcasted_iota(jnp.int32, (tokens, tokens), 0) > lax.broadcasted_iota(
        jnp.int32, (tokens, tokens), 1
    )
    rank = jnp.dot(
        jnp.where(below, 1.0, 0.0).astype(jnp.bfloat16),
        takes.astype(jnp.bfloat16),
        preferred_element_type=jnp.float32,
    )
    spot = (lane - block * slots).astype(jnp.float32)
    place = jnp.where((rank == spot) & (takes > 0.0), 1.0, 0.0)
    pick = place.astype(jnp.bfloat16)

    for copy in shifts:
        copy.wait_recv()

    dispatch = {}
    for f in range(feat):
        at = pl.ds(f * step_f, step_f)
        taken = lax.dot_general(
            pick, arrived[:, at], (((0,), (0,)), ((), ())), preferred_element_type=jnp.float32
        ).astype(jnp.float32)
        for o in list(range(1, n_exp)) + [0]:
            rows = taken[o * slots : (o + 1) * slots].astype(jnp.bfloat16)
            if o == 0:
                recv[0, 0:slots, at] = rows
                continue
            send[o, 0:slots, at] = rows
            dispatch[o, f] = pltpu.make_async_remote_copy(
                src_ref=send.at[o, pl.ds(0, slots), at], dst_ref=recv.at[o, pl.ds(0, slots), at],
                send_sem=disp_send.at[o, f], recv_sem=disp_recv.at[o, f],
                device_id=member(o), device_id_type=MESH,
            )
            dispatch[o, f].start()

    gain_load.wait()
    held = arrived[...].astype(jnp.float32)
    small[0] = jnp.broadcast_to(jnp.sum(held * held, axis=1, keepdims=True), (tokens, 128))
    small[1] = jnp.zeros((tokens, 128), jnp.float32)
    small[1, :, 0:experts] = lax.dot_general(
        held * gain_ref[:, 0:width], router_ref[...], (((1,), (1,)), ((), ())),
        preferred_element_type=jnp.float32, precision=lax.Precision.HIGHEST,
    )

    def to_holders(src, dst, sem):
        copies = [
            pltpu.make_async_remote_copy(
                src_ref=src, dst_ref=dst(o), send_sem=ten_send.at[o, sem], recv_sem=ten_recv.at[o, sem],
                device_id=holder(o), device_id_type=MESH,
            )
            for o in range(1, n_ten)
        ]
        for copy in copies:
            copy.start()
        return copies

    small_copies = to_holders(small, lambda o: small_in.at[o], cols)

    square = jnp.zeros((total, 1), jnp.float32)
    for f in range(feat):
        at = pl.ds(f * step_f, step_f)
        gain = gain_ref[:, at]
        for o in range(n_exp):
            if o > 0:
                dispatch[o, f].wait_recv()
            rows32[pl.ds(o * slots, slots), :] = recv[o, 0:slots, at].astype(jnp.float32)
        rows = rows32[...]
        square += jnp.sum(rows * rows, axis=1, keepdims=True)
        if f == feat - 1:
            squares[...] = jnp.broadcast_to(square, (total, 128))
            square_copies = to_holders(squares, lambda o: squares_in.at[o], cols + 1)
        lifted = (rows * gain).astype(jnp.bfloat16)
        loads[f].wait()
        if f < feat - 1:
            found = jnp.dot(lifted, up[at, :], preferred_element_type=jnp.float32)
            if f == 0:
                inner[...] = found
            else:
                inner[...] += found
    exchange = []
    for c in range(cols):
        units = pl.ds(c * step_c, step_c)
        found = jnp.dot(lifted, up[at, units], preferred_element_type=jnp.float32)
        if feat > 1:
            found += inner[:, units]
        inner[:, units] = found
        part[c] = found.astype(jnp.bfloat16)
        exchange.append(to_holders(part.at[c], lambda o, c=c: parts_in.at[o, c], c))

    for copy in small_copies:
        copy.wait_recv()
    sums, logits = small[0], small[1, :, 0:experts]
    for o in range(1, n_ten):
        sums = sums + small_in[o, 0]
        logits = logits + small_in[o, 1, :, 0:experts]
    full = float(width * n_ten)
    logits = logits * lax.rsqrt(sums[:, 0:1] / full + norm_eps)
    which = lax.broadcasted_iota(jnp.int32, logits.shape, 1)
    scores = []
    for k in range(ids.shape[1]):
        picked = jnp.sum(jnp.where(ids[:, k : k + 1] == which, logits, 0.0), axis=1, keepdims=True)
        scores.append(1.0 / (1.0 + jnp.exp(-picked)))
    norm = scores[0]
    for score in scores[1:]:
        norm = norm + score
    gate = jnp.zeros((tokens, total), jnp.float32)
    for k, score in enumerate(scores):
        gate += jnp.where(ids[:, k : k + 1] == lane_expert, route_scale * score / norm, 0.0)
    gate = gate * place
    coarse = gate.astype(jnp.bfloat16)
    weights[0, :, 0:total] = coarse
    weights[1, :, 0:total] = (gate - coarse.astype(jnp.float32)).astype(jnp.bfloat16)

    for copy in square_copies:
        copy.wait_recv()
    total_sq = squares[...]
    for o in range(1, n_ten):
        total_sq = total_sq + squares_in[o]
    inverse = lax.rsqrt(total_sq[:, 0:1] / full + norm_eps)
    for c in range(cols):
        units = pl.ds(c * step_c, step_c)
        for copy in exchange[c]:
            copy.wait_recv()
        value = inner[:, units]
        for o in range(1, n_ten):
            value = value + parts_in[o, c].astype(jnp.float32)
        value = value * inverse
        active[:, units] = (value / (1.0 + jnp.exp(-value))).astype(jnp.bfloat16)

    loads[feat].wait()
    returns = {}
    for f in range(feat):
        at = pl.ds(f * step_f, step_f)
        made = jnp.dot(active[...], down[:, at], preferred_element_type=jnp.float32)
        for o in list(range(1, n_exp)) + [0]:
            rows = made[o * slots : (o + 1) * slots].astype(jnp.bfloat16)
            if o == 0:
                back[0, 0:slots, at] = rows
                continue
            ret[o, 0:slots, at] = rows
            returns[o, f] = pltpu.make_async_remote_copy(
                src_ref=ret.at[o, pl.ds(0, slots), at], dst_ref=back.at[o, pl.ds(0, slots), at],
                send_sem=ret_send.at[o, f], recv_sem=ret_recv.at[o, f],
                device_id=member(-o), device_id_type=MESH,
            )
            returns[o, f].start()

    for f in range(feat):
        at = pl.ds(f * step_f, step_f)
        for o in range(n_exp):
            if o > 0:
                returns[o, f].wait_recv()
            rows32[pl.ds(o * slots, slots), :] = back[o, 0:slots, at].astype(jnp.float32)
        rows = rows32[...].astype(jnp.bfloat16)
        mixed = jnp.dot(weights[0, :, 0:total], rows, preferred_element_type=jnp.float32)
        mixed += jnp.dot(weights[1, :, 0:total], rows, preferred_element_type=jnp.float32)
        out_ref[:, at] = (arrived[:, at].astype(jnp.float32) + mixed).astype(jnp.bfloat16)

    for copies in [shifts, dispatch.values(), small_copies, square_copies, returns.values()] + exchange:
        for copy in copies:
            copy.wait_send()


def relay(
    sizes, cap,
    stream, ids_hbm, gain_hbm, router_hbm, up_hbm, down_hbm, out_ref,
    ids_ref, up, down, mine, arrived, pool, inner, part, part_in, active, small, small_in, meta, acc, opp_made,
    lhs, spare, pack_out, pack_in, ret_send, ret_in, gain_ref, router_ref,
    load_sem, shift_send, shift_recv, disp_send, disp_recv, ten_send, ten_recv,
    meta_send, meta_recv, rets_send, rets_recv, pack_send, pack_recv,
):
    n_pipe, n_exp, n_ten = sizes
    pipe, expert, tensor = lax.axis_index("pipe"), lax.axis_index("expert"), lax.axis_index("tensor")
    rows, width = arrived.shape[1:]
    experts = router_ref.shape[0]
    bf16, f32 = jnp.bfloat16, jnp.float32
    half = width // 2
    first_part = -(-half // 512) * 256
    subs = [(0, first_part), (first_part, half - first_part)]
    spans = [pl.ds(h * half + at, wide) for h in range(2) for at, wide in subs]
    base = experts + 1
    mate_id = expert + 1 - 2 * lax.rem(expert, 2)

    side = expert // 2
    inside = lax.rem((expert + 1) // 2, 2)
    partner = (pipe, expert + 1 - 2 * lax.rem(expert, 2), tensor)
    across, beyond = (pipe, 2 - side, tensor), (pipe, 3 - 3 * side, tensor)
    holder = (pipe, expert, 1 - tensor)
    after, before = lax.rem(pipe + 1, n_pipe), lax.rem(pipe + n_pipe - 1, n_pipe)
    sections = [(after, expert, tensor), (before, expert, tensor)]

    barrier = pltpu.get_barrier_semaphore()
    for who in sections + [holder, partner]:
        pl.semaphore_signal(barrier, inc=1, device_id=who, device_id_type=MESH)

    @pl.when(inside == 1)
    def _():
        pl.semaphore_signal(barrier, inc=1, device_id=across, device_id_type=MESH)

    mine_load = pltpu.make_async_copy(stream.at[:, 0], mine, load_sem.at[0])
    gain_load = pltpu.make_async_copy(gain_hbm, gain_ref.at[:, pl.ds(0, width)], load_sem.at[1])
    router_load = pltpu.make_async_copy(router_hbm, router_ref, load_sem.at[2])
    down_load = pltpu.make_async_copy(down_hbm.at[0], down, load_sem.at[3])
    ids_load = pltpu.make_async_copy(ids_hbm, ids_ref, load_sem.at[4])
    up_loads = [
        pltpu.make_async_copy(up_hbm.at[0, at], up.at[at], load_sem.at[5 + f])
        for f, at in enumerate(spans)
    ]
    for load in [mine_load, ids_load, gain_load, router_load] + up_loads + [down_load]:
        load.start()

    def heading(c):
        return lax.rem(pipe + 1 + c, 2)

    mine_load.wait()
    pl.semaphore_wait(barrier, 4 + inside)

    def remote(src, dst, send, recv, who):
        return pltpu.make_async_remote_copy(
            src_ref=src, dst_ref=dst, send_sem=send, recv_sem=recv, device_id=who, device_id_type=MESH
        )

    lands = [lax.rem(after + 1, 2), lax.rem(before, 2)]
    shifts = [
        remote(
            mine.at[d], arrived.at[lands[d]], shift_send.at[d], shift_recv.at[lands[d]], sections[d]
        )
        for d in range(2)
    ]
    for copy in shifts:
        copy.start()

    own, mate = pl.ds(0, rows), pl.ds(rows, rows)
    full = float(width * n_ten)
    gain_load.wait()
    router_load.wait()

    lane = lax.broadcasted_iota(jnp.int32, (rows, 128), 1)
    square = (rows, rows)
    eye = jnp.where(
        lax.broadcasted_iota(jnp.int32, square, 0) == lax.broadcasted_iota(jnp.int32, square, 1), 1.0, 0.0
    ).astype(bf16)
    ids_load.wait()
    both = ids_ref[...]
    kind = lax.broadcasted_iota(jnp.int32, (128, rows), 0)
    named = []
    for d in range(2):
        marks = jnp.zeros((128, rows), f32)
        for k in range(both.shape[1]):
            named_id = both[d, k : k + 1, :]
            marks += jnp.where((named_id == kind) | (named_id + base == kind), 1.0, 0.0)
        named.append(
            lax.dot_general(eye, marks.astype(bf16), (((1,), (1,)), ((), ())), preferred_element_type=f32)
        )
    chosen = [jnp.where(heading(c) == 0, named[0], named[1]) for c in range(2)]
    earlier = jnp.where(
        lax.broadcasted_iota(jnp.int32, square, 0) > lax.broadcasted_iota(jnp.int32, square, 1), 1.0, 0.0
    ).astype(bf16)
    slots = [
        jnp.where(mark > 0.0, jnp.dot(earlier, mark.astype(bf16), preferred_element_type=f32), -1.0)
        for mark in chosen
    ]
    slot_id = lax.broadcasted_iota(jnp.int32, square, 1)

    def picks(tile, who):
        wide = lax.broadcasted_iota(jnp.int32, tile.shape, 1)
        slot = jnp.sum(jnp.where(wide == base + who, tile, 0.0), axis=1, keepdims=True)
        low = slot == slot_id.astype(f32)
        high = slot == (slot_id - 4).astype(f32)
        left = jnp.where(low & (slot_id < cap), 1.0, 0.0)
        right = jnp.where((low & (slot_id < 8)) | (high & (slot_id >= 12)), 1.0, 0.0)
        return left.astype(bf16), right.astype(bf16)

    def perform(within):
        started, loaded, exchange = list(shifts), set(), {}

        def go(copy):
            copy.start()
            started.append(copy)

        def rows_to(c, f, src, dst, send, recv, who):
            return remote(
                pool.at[c, *src, spans[f]], pool.at[c, *dst, spans[f]],
                disp_send.at[send, c, f], disp_recv.at[recv, c, f], who,
            )

        def tile_to(c, src, dst, send, recv, who):
            return remote(meta.at[c, *src], meta.at[c, *dst], meta_send.at[send, c], meta_recv.at[recv, c], who)

        def spot(j):
            return pl.ds(j * rows, rows)

        def to_mate(c, f):
            return rows_to(c, f, (0, own), (0, mate), 0, 0, partner)

        def to_other(c, f, j):
            return rows_to(c, f, (0, spot(j)), (1, spot(j)), 1 + j, 1 + j, across)

        def relayed_rows(c, f, j):
            return rows_to(c, f, (1, spot(j)), (1, spot(j)), 3 + j, 1 + j, partner)

        def tile_mate(c):
            return tile_to(c, (0, own), (0, mate), 0, 0, partner)

        def tile_other(c, j):
            return tile_to(c, (0, spot(j)), (1, spot(j)), 1 + j, 1 + j, across)

        def relayed_tile(c, j):
            return tile_to(c, (1, spot(j)), (1, spot(j)), 3 + j, 1 + j, partner)

        def take_in(c):
            remote(mine.at[0], arrived.at[c], shift_send.at[0], shift_recv.at[c], sections[0]).wait_recv()
            for f, at in enumerate(spans):
                pool[c, 0, 0:rows, at] = (arrived[c, :, at].astype(f32) * gain_ref[:, at]).astype(bf16)
            for f in range(len(spans)):
                go(to_mate(c, f))
                if within and c == 0:
                    go(to_other(c, f, 0))
            if within and c == 1:
                send_across(1, 0, 2)
            total = jnp.zeros((rows, 1), f32)
            found = [jnp.zeros((rows, 1), f32) for _ in range(experts)]
            for at in spans:
                held = arrived[c, :, at].astype(f32)
                total += jnp.sum(held * held, axis=1, keepdims=True)
                lifted = held * gain_ref[:, at]
                routes = router_ref[:, at]
                for x in range(experts):
                    found[x] += jnp.sum(lifted * routes[x : x + 1], axis=1, keepdims=True)
            tile = jnp.where(lane == experts, total, 0.0)
            for x in range(experts):
                tile = jnp.where(lane == x, found[x], tile)
            small[c] = tile
            copy = remote(small.at[c], small_in.at[c], ten_send.at[6 + c], ten_recv.at[6 + c], holder)
            go(copy)
            return copy

        def weigh(c, copy):
            copy.wait_recv()
            tile = small[c] + small_in[c]
            inverse = lax.rsqrt(tile[:, experts : experts + 1] / full + norm_eps)
            scores = 1.0 / (1.0 + jnp.exp(-(tile * inverse)))
            scores = jnp.where((chosen[c] > 0.0) & (lane < experts), scores, 0.0)
            norm = jnp.sum(scores, axis=1, keepdims=True)
            tile = jnp.where(lane == experts, inverse, route_scale * scores / norm)
            meta[c, 0, 0:rows] = jnp.where(lane < base, tile, slots[c])
            go(tile_mate(c))
            if within:
                go(tile_other(c, 0))

        def send_across(c, first, end):
            for f in range(first, end):
                go(to_other(c, f, 0))

        def relay_mate(c):
            for f in range(len(spans)):
                to_mate(c, f).wait_recv()
                go(to_other(c, f, 1))

        def relay_mate_tile(c):
            tile_mate(c).wait_recv()
            go(tile_other(c, 1))

        def relay_rows(c, j):
            for f in range(len(spans)):
                copy = relayed_rows(c, f, j)
                copy.wait_recv()
                go(copy)

        def relay_tile(c, j):
            copy = relayed_tile(c, j)
            copy.wait_recv()
            go(copy)

        def go_up(p, ready=None):
            c, g, first, many = passes[p]
            band = pl.ds(first * rows, many * rows)
            if "up" not in loaded:
                for load in up_loads:
                    load.wait()
                loaded.add("up")
            if ready is not None:
                heard(ready)
            if within:
                found = jnp.dot(pool[c, g, band, :], up[...], preferred_element_type=f32)
            else:
                bounds = [0, width - half, width] if g == 0 else [0, width]
                for low, high in zip(bounds, bounds[1:]):
                    for f in range(2 * low // half, 2 * high // half):
                        (to_mate(c, f) if g == 0 else relayed_rows(c, f, first)).wait_recv()
                    more = jnp.dot(
                        pool[c, g, band, low:high], up[low:high, :], preferred_element_type=f32
                    )
                    found = more if low == 0 else found + more
            if ready is not None:
                activate(ready)
            inner[c, g, band, :] = found
            part[c, g, band, :] = found.astype(bf16)
            exchange[p] = remote(
                part.at[c, g, band], part_in.at[c, g, band], ten_send.at[p], ten_recv.at[p], holder
            )
            go(exchange[p])

        def heard(p):
            c, g, first, many = passes[p]
            if not within:
                (tile_mate(c) if g == 0 else relayed_tile(c, first)).wait_recv()
            exchange[p].wait_recv()
            loaded.add(p)

        def activate(p):
            c, g, first, many = passes[p]
            band = pl.ds(first * rows, many * rows)
            tile = meta[c, g, band]
            wide = lax.broadcasted_iota(jnp.int32, tile.shape, 1)
            gate = jnp.sum(jnp.where(wide == expert, tile, 0.0), axis=1, keepdims=True)
            inverse = tile[:, experts : experts + 1]
            value = (inner[c, g, band, :] + part_in[c, g, band, :].astype(f32)) * inverse
            value = (gate * (value / (1.0 + jnp.exp(-value)))).astype(bf16)
            if within:
                active[c, g, band, :] = value
                return
            k = 0 if g == 0 else 1 + first
            for h, pick in enumerate(picks(tile[-rows:], expert)):
                if g == 0:
                    lhs[c, k, h, rows : 2 * rows, :] = value[0:rows]
                lhs[c, k, h, 0:rows, :] = lax.dot_general(
                    pick, value[-rows:], (((0,), (0,)), ((), ())), preferred_element_type=f32
                ).astype(bf16)

        def packed(c, k, b):
            return remote(
                pack_out.at[c, k, b], pack_in.at[c, k, b], pack_send.at[k, c, b], pack_recv.at[k, c, b], partner
            )

        def go_down(p):
            c, g, first, many = passes[p]
            band = pl.ds(first * rows, many * rows)
            if p not in loaded:
                heard(p)
                activate(p)
            if "down" not in loaded:
                down_load.wait()
                loaded.add("down")
            k = 0 if g == 0 else 1 + first

            def deliver(f, made):
                at = spans[f]
                h, (low, wide) = f // 2, subs[f % 2]
                if within and g == 0:
                    acc[c, :, at] = arrived[c, :, at].astype(f32) + made[0:rows]
                    ret_send[c, 0, :, at] = made[rows:].astype(bf16)
                    go(back_to_mate(c, f))
                elif within:
                    for j in range(2):
                        opp_made[c, j, :, at] = made[j * rows : (j + 1) * rows]
                else:
                    if g == 0:
                        acc[c, :, at] = arrived[c, :, at].astype(f32) + made[rows:]
                    local = pl.ds(low, wide)
                    pack_out[c, k, h, :, local] = made[0:8].astype(bf16)
                    if h == 0:
                        spare[c, k, :, local] = made[8:16]
                    else:
                        pack_out[c, k, 2, :, local] = (spare[c, k, :, local] + made[8:16]).astype(bf16)
                    if f == 1:
                        go(packed(c, k, 0))
                    if f == 3:
                        go(packed(c, k, 2))
                        go(packed(c, k, 1))

            last = None
            for f, at in enumerate(spans):
                left = active[c, g, band, :] if within else lhs[c, k, f // 2, 0 : many * rows, :]
                made = jnp.dot(left, down[:, at], preferred_element_type=f32)
                if last is not None:
                    deliver(f - 1, last)
                last = made
            deliver(len(spans) - 1, last)

        def spread(c, k, f, pick):
            h, (low, wide) = f // 2, subs[f % 2]
            local = pl.ds(low, wide)
            if f == 0:
                packed(c, k, 0).wait_recv()
                packed(c, k, 2).wait_recv()
            if f == 2:
                packed(c, k, 1).wait_recv()
            got = jnp.concatenate(
                [pack_in[c, k, h, :, local].astype(f32), pack_in[c, k, 2, :, local].astype(f32)], axis=0
            ).astype(bf16)
            return jnp.dot(pick[h], got, preferred_element_type=f32)

        def absorb(c):
            pick = picks(meta[c, 0, 0:rows], mate_id)
            for f, at in enumerate(spans):
                acc[c, :, at] += spread(c, 0, f, pick)

        def back_to_mate(c, f):
            at = spans[f]
            return remote(
                ret_send.at[c, 0, :, at], ret_in.at[c, 0, :, at],
                rets_send.at[0, c, f], rets_recv.at[0, c, f], partner,
            )

        def sum_home(c, f, j):
            at = spans[f]
            return remote(
                ret_send.at[c, 1 + j, :, at], ret_in.at[c, 1, :, at],
                rets_send.at[1 + j, c, f], rets_recv.at[1, c, f], beyond if j else across,
            )

        def combine(c, j):
            pick = picks(meta[c, 1, spot(j)], mate_id)
            for f, at in enumerate(spans):
                ret_send[c, 1 + j, :, at] = (
                    opp_made[c, j, :, at] + spread(c, 1 + j, f, pick)
                ).astype(bf16)
                go(sum_home(c, f, j))

        def finish(c):
            for f, at in enumerate(spans):
                total = acc[c, :, at]
                if not within:
                    back_to_mate(c, f).wait_recv()
                    total += ret_in[c, 0, :, at].astype(f32)
                sum_home(c, f, 0).wait_recv()
                total += ret_in[c, 1, :, at].astype(f32)
                out_ref[heading(c), :, at] = total.astype(bf16)

        near = take_in(0)
        far = take_in(1)
        if within:
            passes = [(0, 0, 0, 2), (0, 1, 0, 2), (1, 0, 0, 2), (1, 1, 0, 2)]
            weigh(0, near)
            relay_rows(0, 0)
            relay_mate(0)
            relay_mate(1)
            relay_mate_tile(0)
            send_across(1, 2, 4)
            weigh(1, far)
            go_up(0)
            relay_rows(0, 1)
            relay_tile(0, 0)
            relay_mate_tile(1)
            go_up(1)
            relay_rows(1, 1)
            relay_tile(0, 1)
            go_up(2)
            relay_tile(1, 1)
            relay_rows(1, 0)
            go_up(3)
            relay_tile(1, 0)
            go_down(1)
            go_down(0)
            go_down(2)
            absorb(0)
            absorb(1)
            combine(0, 0)
            go_down(3)
            combine(0, 1)
            combine(1, 1)
            combine(1, 0)
        else:
            passes = [(0, 0, 0, 2), (1, 0, 0, 2), (0, 1, 0, 1), (0, 1, 1, 1), (1, 1, 1, 1), (1, 1, 0, 1)]
            weigh(0, near)
            go_up(0)
            weigh(1, far)
            go_up(1)
            go_up(2)
            go_down(0)
            go_down(1)
            go_up(3)
            go_down(2)
            go_up(4)
            go_down(3)
            go_up(5)
            go_down(4)
            go_down(5)
        finish(0)
        finish(1)
        for copy in started:
            copy.wait_send()

    @pl.when(inside == 1)
    def _():
        perform(True)

    @pl.when(inside == 0)
    def _():
        perform(False)


def relayed(sizes, stream, expert_ids, norm_gain, router, w_up, w_down):
    n_pipe, n_exp, n_ten = sizes
    rows, width = stream.shape[2:]
    experts, fanout = router.shape[2], expert_ids.shape[3]
    hidden_units = w_up.shape[2]
    cap = 3 * rows * fanout // (2 * experts)
    pieces = 4
    bf16, f32 = jnp.bfloat16, jnp.float32
    dma = pltpu.SemaphoreType.DMA
    vmem = pl.BlockSpec(memory_space=pltpu.VMEM)
    hbm = pl.BlockSpec(memory_space=pl.ANY)
    result = pl.pallas_call(
        functools.partial(relay, sizes, cap),
        out_shape=pltpu.VMEM((2, rows, width), bf16),
        in_specs=[hbm] * 6,
        out_specs=vmem,
        scratch_shapes=[
            pltpu.VMEM((2, fanout, rows), jnp.int32),
            pltpu.VMEM((width, hidden_units), bf16),
            pltpu.VMEM((hidden_units, width), bf16),
            pltpu.VMEM((2, rows, width), bf16),
            pltpu.VMEM((2, rows, width), bf16),
            pltpu.VMEM((2, 2, 2 * rows, width), bf16),
            pltpu.VMEM((2, 2, 2 * rows, hidden_units), f32),
            pltpu.VMEM((2, 2, 2 * rows, hidden_units), bf16),
            pltpu.VMEM((2, 2, 2 * rows, hidden_units), bf16),
            pltpu.VMEM((2, 2, 2 * rows, hidden_units), bf16),
            pltpu.VMEM((2, rows, 128), f32),
            pltpu.VMEM((2, rows, 128), f32),
            pltpu.VMEM((2, 2, 2 * rows, 128), f32),
            pltpu.VMEM((2, rows, width), f32),
            pltpu.VMEM((2, 2, rows, width), f32),
            pltpu.VMEM((2, 3, 2, 2 * rows, hidden_units), bf16),
            pltpu.VMEM((2, 3, 8, width // 2), f32),
            pltpu.VMEM((2, 3, 3, 8, width // 2), bf16),
            pltpu.VMEM((2, 3, 3, 8, width // 2), bf16),
            pltpu.VMEM((2, 3, rows, width), bf16),
            pltpu.VMEM((2, 2, rows, width), bf16),
            pltpu.VMEM((1, width + 1024), f32),
            pltpu.VMEM((experts, width), f32),
            dma((5 + pieces,)),
            dma((2,)),
            dma((2,)),
            dma((5, 2, pieces)),
            dma((3, 2, pieces)),
            dma((8,)),
            dma((8,)),
            dma((5, 2)),
            dma((3, 2)),
            dma((3, 2, pieces)),
            dma((2, 2, pieces)),
            dma((3, 2, 3)),
            dma((3, 2, 3)),
        ],
        compiler_params=pltpu.CompilerParams(
            collective_id=0, has_side_effects=True, vmem_limit_bytes=67043328 - 4 * rows * width - 16384
        ),
    )(stream, expert_ids[:, 0].transpose(0, 2, 1), norm_gain, router[0].T, w_up, w_down)
    return result.reshape(2, 1, rows, width)


def shards(sizes, stream, expert_ids, norm_gain, router, w_up, w_down):
    n_pipe, n_exp, n_ten = sizes
    if n_exp == 4 and n_ten == 2 and n_pipe > 1 and n_pipe % 2 == 0 and router.shape[2] == n_exp:
        return relayed(sizes, stream, expert_ids, norm_gain, router, w_up, w_down)
    tok_rows, width = stream.shape[2:]
    fanout = expert_ids.shape[-1]
    experts = router.shape[2]
    hidden_units = w_up.shape[2]
    tokens = 2 * tok_rows
    capacity = 3 * tok_rows * fanout // (2 * experts)
    slots = -(-2 * capacity // 8) * 8
    total = n_exp * slots
    feat = pieces_of(width, 4)
    cols = pieces_of(hidden_units, 4)
    bf16, f32 = jnp.bfloat16, jnp.float32
    dma = pltpu.SemaphoreType.DMA
    vmem = pl.BlockSpec(memory_space=pltpu.VMEM)
    hbm = pl.BlockSpec(memory_space=pl.ANY)
    result = pl.pallas_call(
        functools.partial(layer, sizes, slots, feat, cols),
        out_shape=jax.ShapeDtypeStruct((tokens, width), bf16),
        in_specs=[hbm, vmem, hbm, vmem, hbm, hbm],
        out_specs=vmem,
        scratch_shapes=[
            pltpu.VMEM((width, hidden_units), bf16),
            pltpu.VMEM((hidden_units, width), bf16),
            pltpu.VMEM((tokens, width), bf16),
            pltpu.VMEM((n_exp, -(-slots // 16) * 16, width), bf16),
            pltpu.VMEM((n_exp, -(-slots // 16) * 16, width), bf16),
            pltpu.VMEM((total, width // feat), f32),
            pltpu.VMEM((total, hidden_units), f32),
            pltpu.VMEM((cols, total, hidden_units // cols), bf16),
            pltpu.VMEM((n_ten, cols, total, hidden_units // cols), bf16),
            pltpu.VMEM((total, hidden_units), bf16),
            pltpu.VMEM((total, 128), f32),
            pltpu.VMEM((n_ten, total, 128), f32),
            pltpu.VMEM((2, tokens, 128), f32),
            pltpu.VMEM((n_ten, 2, tokens, 128), f32),
            pltpu.VMEM((n_exp, -(-slots // 16) * 16, width), bf16),
            pltpu.VMEM((n_exp, -(-slots // 16) * 16, width), bf16),
            pltpu.VMEM((2, tokens, -(-total // 128) * 128), bf16),
            pltpu.VMEM((1, width + 1024), f32),
            dma((feat + 2,)),
            dma((2,)),
            dma((2,)),
            dma((n_exp, feat)),
            dma((n_exp, feat)),
            dma((n_ten, cols + 2)),
            dma((n_ten, cols + 2)),
            dma((n_exp, feat)),
            dma((n_exp, feat)),
        ],
        compiler_params=pltpu.CompilerParams(
            collective_id=0, has_side_effects=True, vmem_limit_bytes=60 * 1024 * 1024
        ),
    )(stream, expert_ids.reshape(tokens, fanout), norm_gain, router[0].T, w_up, w_down)
    return result.reshape(2, 1, tok_rows, width)


def solution(mesh):
    sizes = tuple(mesh.shape[axis] for axis in ("pipe", "expert", "tensor"))
    return jax.shard_map(
        functools.partial(shards, sizes),
        mesh=mesh,
        in_specs=(
            P(None, "pipe", "expert", "tensor"),
            P(None, "pipe", "expert", None),
            P("pipe", "tensor"),
            P("pipe", "tensor", None),
            P("expert", "tensor", None),
            P("expert", None, "tensor"),
        ),
        out_specs=P(None, "pipe", "expert", "tensor"),
        check_vma=False,
    )
```

```python
import functools

import jax
import jax.numpy as jnp
from jax import lax
from jax.experimental import pallas as pl
from jax.experimental.pallas import tpu as pltpu
from jax.sharding import PartitionSpec as P

norm_eps = 1e-06
route_scale = 2.5
MESH = pl.DeviceIdType.MESH


def pieces_of(width, most):
    for count in range(most, 0, -1):
        if width % (count * 128) == 0:
            return count
    return 1


def layer(
    sizes, slots, feat, cols,
    stream, ids_ref, gain_hbm, router_ref, up_hbm, down_hbm, out_ref,
    up, down, arrived, send, recv, rows32, inner, part, parts_in, active, squares, squares_in,
    small, small_in, ret, back, weights, gain_ref,
    load_sem, shift_send, shift_recv, disp_send, disp_recv, ten_send, ten_recv, ret_send, ret_recv,
):
    n_pipe, n_exp, n_ten = sizes
    pipe, expert, tensor = lax.axis_index("pipe"), lax.axis_index("expert"), lax.axis_index("tensor")
    tokens, width = arrived.shape
    half = tokens // 2
    hidden_units = up.shape[1]
    experts = router_ref.shape[0]
    step_f, step_c = width // feat, hidden_units // cols

    def section(by):
        return (lax.rem(pipe + by + n_pipe, n_pipe), expert, tensor)

    def member(by):
        return (pipe, lax.rem(expert + by + n_exp, n_exp), tensor)

    def holder(by):
        return (pipe, expert, lax.rem(tensor + by + n_ten, n_ten))

    barrier = pltpu.get_barrier_semaphore()
    greeted = [section(1), section(-1)]
    greeted += [member(o) for o in range(1, n_exp)] + [holder(o) for o in range(1, n_ten)]
    for who in greeted:
        pl.semaphore_signal(barrier, inc=1, device_id=who, device_id_type=MESH)

    loads = []
    for f in range(feat):
        at = pl.ds(f * step_f, step_f)
        loads.append(pltpu.make_async_copy(up_hbm.at[0, at], up.at[at], load_sem.at[f]))
    loads.append(pltpu.make_async_copy(down_hbm.at[0], down, load_sem.at[feat]))
    gain_load = pltpu.make_async_copy(
        gain_hbm, gain_ref.at[:, pl.ds(0, width)], load_sem.at[feat + 1]
    )
    gain_load.start()
    for load in loads:
        load.start()
    pl.semaphore_wait(barrier, len(greeted))

    shifts = [
        pltpu.make_async_remote_copy(
            src_ref=stream.at[d, 0], dst_ref=arrived.at[pl.ds(d * half, half)],
            send_sem=shift_send.at[d], recv_sem=shift_recv.at[d],
            device_id=section(1 - 2 * d), device_id_type=MESH,
        )
        for d in range(2)
    ]
    for copy in shifts:
        copy.start()

    ids = ids_ref[...]
    total = n_exp * slots
    lane = lax.broadcasted_iota(jnp.int32, (tokens, total), 1)
    block = lane // slots
    lane_expert = lax.rem(block + expert, n_exp)
    takes = jnp.zeros((tokens, total), jnp.float32)
    for k in range(ids.shape[1]):
        takes += jnp.where(ids[:, k : k + 1] == lane_expert, 1.0, 0.0)
    below = lax.broadcasted_iota(jnp.int32, (tokens, tokens), 0) > lax.broadcasted_iota(
        jnp.int32, (tokens, tokens), 1
    )
    rank = jnp.dot(
        jnp.where(below, 1.0, 0.0).astype(jnp.bfloat16),
        takes.astype(jnp.bfloat16),
        preferred_element_type=jnp.float32,
    )
    spot = (lane - block * slots).astype(jnp.float32)
    place = jnp.where((rank == spot) & (takes > 0.0), 1.0, 0.0)
    pick = place.astype(jnp.bfloat16)

    for copy in shifts:
        copy.wait_recv()

    dispatch = {}
    for f in range(feat):
        at = pl.ds(f * step_f, step_f)
        taken = lax.dot_general(
            pick, arrived[:, at], (((0,), (0,)), ((), ())), preferred_element_type=jnp.float32
        ).astype(jnp.float32)
        for o in list(range(1, n_exp)) + [0]:
            rows = taken[o * slots : (o + 1) * slots].astype(jnp.bfloat16)
            if o == 0:
                recv[0, 0:slots, at] = rows
                continue
            send[o, 0:slots, at] = rows
            dispatch[o, f] = pltpu.make_async_remote_copy(
                src_ref=send.at[o, pl.ds(0, slots), at], dst_ref=recv.at[o, pl.ds(0, slots), at],
                send_sem=disp_send.at[o, f], recv_sem=disp_recv.at[o, f],
                device_id=member(o), device_id_type=MESH,
            )
            dispatch[o, f].start()

    gain_load.wait()
    held = arrived[...].astype(jnp.float32)
    small[0] = jnp.broadcast_to(jnp.sum(held * held, axis=1, keepdims=True), (tokens, 128))
    small[1] = jnp.zeros((tokens, 128), jnp.float32)
    small[1, :, 0:experts] = lax.dot_general(
        held * gain_ref[:, 0:width], router_ref[...], (((1,), (1,)), ((), ())),
        preferred_element_type=jnp.float32, precision=lax.Precision.HIGHEST,
    )

    def to_holders(src, dst, sem):
        copies = [
            pltpu.make_async_remote_copy(
                src_ref=src, dst_ref=dst(o), send_sem=ten_send.at[o, sem], recv_sem=ten_recv.at[o, sem],
                device_id=holder(o), device_id_type=MESH,
            )
            for o in range(1, n_ten)
        ]
        for copy in copies:
            copy.start()
        return copies

    small_copies = to_holders(small, lambda o: small_in.at[o], cols)

    square = jnp.zeros((total, 1), jnp.float32)
    for f in range(feat):
        at = pl.ds(f * step_f, step_f)
        gain = gain_ref[:, at]
        for o in range(n_exp):
            if o > 0:
                dispatch[o, f].wait_recv()
            rows32[pl.ds(o * slots, slots), :] = recv[o, 0:slots, at].astype(jnp.float32)
        rows = rows32[...]
        square += jnp.sum(rows * rows, axis=1, keepdims=True)
        if f == feat - 1:
            squares[...] = jnp.broadcast_to(square, (total, 128))
            square_copies = to_holders(squares, lambda o: squares_in.at[o], cols + 1)
        lifted = (rows * gain).astype(jnp.bfloat16)
        loads[f].wait()
        if f < feat - 1:
            found = jnp.dot(lifted, up[at, :], preferred_element_type=jnp.float32)
            if f == 0:
                inner[...] = found
            else:
                inner[...] += found
    exchange = []
    for c in range(cols):
        units = pl.ds(c * step_c, step_c)
        found = jnp.dot(lifted, up[at, units], preferred_element_type=jnp.float32)
        if feat > 1:
            found += inner[:, units]
        inner[:, units] = found
        part[c] = found.astype(jnp.bfloat16)
        exchange.append(to_holders(part.at[c], lambda o, c=c: parts_in.at[o, c], c))

    for copy in small_copies:
        copy.wait_recv()
    sums, logits = small[0], small[1, :, 0:experts]
    for o in range(1, n_ten):
        sums = sums + small_in[o, 0]
        logits = logits + small_in[o, 1, :, 0:experts]
    full = float(width * n_ten)
    logits = logits * lax.rsqrt(sums[:, 0:1] / full + norm_eps)
    which = lax.broadcasted_iota(jnp.int32, logits.shape, 1)
    scores = []
    for k in range(ids.shape[1]):
        picked = jnp.sum(jnp.where(ids[:, k : k + 1] == which, logits, 0.0), axis=1, keepdims=True)
        scores.append(1.0 / (1.0 + jnp.exp(-picked)))
    norm = scores[0]
    for score in scores[1:]:
        norm = norm + score
    gate = jnp.zeros((tokens, total), jnp.float32)
    for k, score in enumerate(scores):
        gate += jnp.where(ids[:, k : k + 1] == lane_expert, route_scale * score / norm, 0.0)
    gate = gate * place
    coarse = gate.astype(jnp.bfloat16)
    weights[0, :, 0:total] = coarse
    weights[1, :, 0:total] = (gate - coarse.astype(jnp.float32)).astype(jnp.bfloat16)

    for copy in square_copies:
        copy.wait_recv()
    total_sq = squares[...]
    for o in range(1, n_ten):
        total_sq = total_sq + squares_in[o]
    inverse = lax.rsqrt(total_sq[:, 0:1] / full + norm_eps)
    for c in range(cols):
        units = pl.ds(c * step_c, step_c)
        for copy in exchange[c]:
            copy.wait_recv()
        value = inner[:, units]
        for o in range(1, n_ten):
            value = value + parts_in[o, c].astype(jnp.float32)
        value = value * inverse
        active[:, units] = (value / (1.0 + jnp.exp(-value))).astype(jnp.bfloat16)

    loads[feat].wait()
    returns = {}
    for f in range(feat):
        at = pl.ds(f * step_f, step_f)
        made = jnp.dot(active[...], down[:, at], preferred_element_type=jnp.float32)
        for o in list(range(1, n_exp)) + [0]:
            rows = made[o * slots : (o + 1) * slots].astype(jnp.bfloat16)
            if o == 0:
                back[0, 0:slots, at] = rows
                continue
            ret[o, 0:slots, at] = rows
            returns[o, f] = pltpu.make_async_remote_copy(
                src_ref=ret.at[o, pl.ds(0, slots), at], dst_ref=back.at[o, pl.ds(0, slots), at],
                send_sem=ret_send.at[o, f], recv_sem=ret_recv.at[o, f],
                device_id=member(-o), device_id_type=MESH,
            )
            returns[o, f].start()

    for f in range(feat):
        at = pl.ds(f * step_f, step_f)
        for o in range(n_exp):
            if o > 0:
                returns[o, f].wait_recv()
            rows32[pl.ds(o * slots, slots), :] = back[o, 0:slots, at].astype(jnp.float32)
        rows = rows32[...].astype(jnp.bfloat16)
        mixed = jnp.dot(weights[0, :, 0:total], rows, preferred_element_type=jnp.float32)
        mixed += jnp.dot(weights[1, :, 0:total], rows, preferred_element_type=jnp.float32)
        out_ref[:, at] = (arrived[:, at].astype(jnp.float32) + mixed).astype(jnp.bfloat16)

    for copies in [shifts, dispatch.values(), small_copies, square_copies, returns.values()] + exchange:
        for copy in copies:
            copy.wait_send()


def relay(
    sizes, cap,
    stream, ids_hbm, gain_hbm, router_hbm, up_hbm, down_hbm, out_ref,
    ids_ref, up, down, mine, arrived, pool, inner, part, part_in, active, small, small_in, meta, acc, opp_made,
    lhs, spare, pack_out, pack_in, ret_send, ret_in, gain_ref, router_ref,
    load_sem, shift_send, shift_recv, disp_send, disp_recv, ten_send, ten_recv,
    meta_send, meta_recv, rets_send, rets_recv, pack_send, pack_recv,
):
    n_pipe, n_exp, n_ten = sizes
    pipe, expert, tensor = lax.axis_index("pipe"), lax.axis_index("expert"), lax.axis_index("tensor")
    rows, width = arrived.shape[1:]
    experts = router_ref.shape[0]
    bf16, f32 = jnp.bfloat16, jnp.float32
    half = width // 2
    first_part = -(-half // 512) * 256
    subs = [(0, first_part), (first_part, half - first_part)]
    spans = [pl.ds(h * half + at, wide) for h in range(2) for at, wide in subs]
    base = experts + 1
    mate_id = expert + 1 - 2 * lax.rem(expert, 2)

    side = expert // 2
    inside = lax.rem((expert + 1) // 2, 2)
    partner = (pipe, expert + 1 - 2 * lax.rem(expert, 2), tensor)
    across, beyond = (pipe, 2 - side, tensor), (pipe, 3 - 3 * side, tensor)
    holder = (pipe, expert, 1 - tensor)
    after, before = lax.rem(pipe + 1, n_pipe), lax.rem(pipe + n_pipe - 1, n_pipe)
    sections = [(after, expert, tensor), (before, expert, tensor)]

    barrier = pltpu.get_barrier_semaphore()
    for who in sections + [holder, partner]:
        pl.semaphore_signal(barrier, inc=1, device_id=who, device_id_type=MESH)

    @pl.when(inside == 1)
    def _():
        pl.semaphore_signal(barrier, inc=1, device_id=across, device_id_type=MESH)

    mine_load = pltpu.make_async_copy(stream.at[:, 0], mine, load_sem.at[0])
    gain_load = pltpu.make_async_copy(gain_hbm, gain_ref.at[:, pl.ds(0, width)], load_sem.at[1])
    router_load = pltpu.make_async_copy(router_hbm, router_ref, load_sem.at[2])
    down_load = pltpu.make_async_copy(down_hbm.at[0], down, load_sem.at[3])
    ids_load = pltpu.make_async_copy(ids_hbm, ids_ref, load_sem.at[4])
    up_loads = [
        pltpu.make_async_copy(up_hbm.at[0, at], up.at[at], load_sem.at[5 + f])
        for f, at in enumerate(spans)
    ]
    for load in [mine_load, ids_load, gain_load, router_load] + up_loads + [down_load]:
        load.start()

    def heading(c):
        return lax.rem(pipe + 1 + c, 2)

    mine_load.wait()
    pl.semaphore_wait(barrier, 4 + inside)

    def remote(src, dst, send, recv, who):
        return pltpu.make_async_remote_copy(
            src_ref=src, dst_ref=dst, send_sem=send, recv_sem=recv, device_id=who, device_id_type=MESH
        )

    lands = [lax.rem(after + 1, 2), lax.rem(before, 2)]
    shifts = [
        remote(
            mine.at[d], arrived.at[lands[d]], shift_send.at[d], shift_recv.at[lands[d]], sections[d]
        )
        for d in range(2)
    ]
    for copy in shifts:
        copy.start()

    own, mate = pl.ds(0, rows), pl.ds(rows, rows)
    full = float(width * n_ten)
    gain_load.wait()
    router_load.wait()

    lane = lax.broadcasted_iota(jnp.int32, (rows, 128), 1)
    square = (rows, rows)
    eye = jnp.where(
        lax.broadcasted_iota(jnp.int32, square, 0) == lax.broadcasted_iota(jnp.int32, square, 1), 1.0, 0.0
    ).astype(bf16)
    ids_load.wait()
    both = ids_ref[...]
    kind = lax.broadcasted_iota(jnp.int32, (128, rows), 0)
    named = []
    for d in range(2):
        marks = jnp.zeros((128, rows), f32)
        for k in range(both.shape[1]):
            named_id = both[d, k : k + 1, :]
            marks += jnp.where((named_id == kind) | (named_id + base == kind), 1.0, 0.0)
        named.append(
            lax.dot_general(eye, marks.astype(bf16), (((1,), (1,)), ((), ())), preferred_element_type=f32)
        )
    chosen = [jnp.where(heading(c) == 0, named[0], named[1]) for c in range(2)]
    earlier = jnp.where(
        lax.broadcasted_iota(jnp.int32, square, 0) > lax.broadcasted_iota(jnp.int32, square, 1), 1.0, 0.0
    ).astype(bf16)
    slots = [
        jnp.where(mark > 0.0, jnp.dot(earlier, mark.astype(bf16), preferred_element_type=f32), -1.0)
        for mark in chosen
    ]
    slot_id = lax.broadcasted_iota(jnp.int32, square, 1)

    def picks(tile, who):
        wide = lax.broadcasted_iota(jnp.int32, tile.shape, 1)
        slot = jnp.sum(jnp.where(wide == base + who, tile, 0.0), axis=1, keepdims=True)
        low = slot == slot_id.astype(f32)
        high = slot == (slot_id - 4).astype(f32)
        left = jnp.where(low & (slot_id < cap), 1.0, 0.0)
        right = jnp.where((low & (slot_id < 8)) | (high & (slot_id >= 12)), 1.0, 0.0)
        return left.astype(bf16), right.astype(bf16)

    def perform(within):
        started, loaded, exchange = list(shifts), set(), {}

        def go(copy):
            copy.start()
            started.append(copy)

        def rows_to(c, f, src, dst, send, recv, who):
            return remote(
                pool.at[c, *src, spans[f]], pool.at[c, *dst, spans[f]],
                disp_send.at[send, c, f], disp_recv.at[recv, c, f], who,
            )

        def tile_to(c, src, dst, send, recv, who):
            return remote(meta.at[c, *src], meta.at[c, *dst], meta_send.at[send, c], meta_recv.at[recv, c], who)

        def spot(j):
            return pl.ds(j * rows, rows)

        def to_mate(c, f):
            return rows_to(c, f, (0, own), (0, mate), 0, 0, partner)

        def to_other(c, f, j):
            return rows_to(c, f, (0, spot(j)), (1, spot(j)), 1 + j, 1 + j, across)

        def relayed_rows(c, f, j):
            return rows_to(c, f, (1, spot(j)), (1, spot(j)), 3 + j, 1 + j, partner)

        def tile_mate(c):
            return tile_to(c, (0, own), (0, mate), 0, 0, partner)

        def tile_other(c, j):
            return tile_to(c, (0, spot(j)), (1, spot(j)), 1 + j, 1 + j, across)

        def relayed_tile(c, j):
            return tile_to(c, (1, spot(j)), (1, spot(j)), 3 + j, 1 + j, partner)

        def take_in(c):
            remote(mine.at[0], arrived.at[c], shift_send.at[0], shift_recv.at[c], sections[0]).wait_recv()
            for f, at in enumerate(spans):
                pool[c, 0, 0:rows, at] = (arrived[c, :, at].astype(f32) * gain_ref[:, at]).astype(bf16)
            for f in range(len(spans)):
                go(to_mate(c, f))
                if within and c == 0:
                    go(to_other(c, f, 0))
            if within and c == 1:
                send_across(1, 0, 2)
            total = jnp.zeros((rows, 1), f32)
            found = [jnp.zeros((rows, 1), f32) for _ in range(experts)]
            for at in spans:
                held = arrived[c, :, at].astype(f32)
                total += jnp.sum(held * held, axis=1, keepdims=True)
                lifted = held * gain_ref[:, at]
                routes = router_ref[:, at]
                for x in range(experts):
                    found[x] += jnp.sum(lifted * routes[x : x + 1], axis=1, keepdims=True)
            tile = jnp.where(lane == experts, total, 0.0)
            for x in range(experts):
                tile = jnp.where(lane == x, found[x], tile)
            small[c] = tile
            copy = remote(small.at[c], small_in.at[c], ten_send.at[6 + c], ten_recv.at[6 + c], holder)
            go(copy)
            return copy

        def weigh(c, copy):
            copy.wait_recv()
            tile = small[c] + small_in[c]
            inverse = lax.rsqrt(tile[:, experts : experts + 1] / full + norm_eps)
            scores = 1.0 / (1.0 + jnp.exp(-(tile * inverse)))
            scores = jnp.where((chosen[c] > 0.0) & (lane < experts), scores, 0.0)
            norm = jnp.sum(scores, axis=1, keepdims=True)
            tile = jnp.where(lane == experts, inverse, route_scale * scores / norm)
            meta[c, 0, 0:rows] = jnp.where(lane < base, tile, slots[c])
            go(tile_mate(c))
            if within:
                go(tile_other(c, 0))

        def send_across(c, first, end):
            for f in range(first, end):
                go(to_other(c, f, 0))

        def relay_mate(c):
            for f in range(len(spans)):
                to_mate(c, f).wait_recv()
                go(to_other(c, f, 1))

        def relay_mate_tile(c):
            tile_mate(c).wait_recv()
            go(tile_other(c, 1))

        def relay_rows(c, j):
            for f in range(len(spans)):
                copy = relayed_rows(c, f, j)
                copy.wait_recv()
                go(copy)

        def relay_tile(c, j):
            copy = relayed_tile(c, j)
            copy.wait_recv()
            go(copy)

        def go_up(p, ready=None):
            c, g, first, many = passes[p]
            band = pl.ds(first * rows, many * rows)
            if "up" not in loaded:
                for load in up_loads:
                    load.wait()
                loaded.add("up")
            if ready is not None:
                heard(ready)
            if within:
                found = jnp.dot(pool[c, g, band, :], up[...], preferred_element_type=f32)
            else:
                bounds = [0, width - half, width] if g == 0 else [0, width]
                for low, high in zip(bounds, bounds[1:]):
                    for f in range(2 * low // half, 2 * high // half):
                        (to_mate(c, f) if g == 0 else relayed_rows(c, f, first)).wait_recv()
                    more = jnp.dot(
                        pool[c, g, band, low:high], up[low:high, :], preferred_element_type=f32
                    )
                    found = more if low == 0 else found + more
            if ready is not None:
                activate(ready)
            inner[c, g, band, :] = found
            part[c, g, band, :] = found.astype(bf16)
            exchange[p] = remote(
                part.at[c, g, band], part_in.at[c, g, band], ten_send.at[p], ten_recv.at[p], holder
            )
            go(exchange[p])

        def heard(p):
            c, g, first, many = passes[p]
            if not within:
                (tile_mate(c) if g == 0 else relayed_tile(c, first)).wait_recv()
            exchange[p].wait_recv()
            loaded.add(p)

        def activate(p):
            c, g, first, many = passes[p]
            band = pl.ds(first * rows, many * rows)
            tile = meta[c, g, band]
            wide = lax.broadcasted_iota(jnp.int32, tile.shape, 1)
            gate = jnp.sum(jnp.where(wide == expert, tile, 0.0), axis=1, keepdims=True)
            inverse = tile[:, experts : experts + 1]
            value = (inner[c, g, band, :] + part_in[c, g, band, :].astype(f32)) * inverse
            value = (gate * (value / (1.0 + jnp.exp(-value)))).astype(bf16)
            if within:
                active[c, g, band, :] = value
                return
            k = 0 if g == 0 else 1 + first
            for h, pick in enumerate(picks(tile[-rows:], expert)):
                if g == 0:
                    lhs[c, k, h, rows : 2 * rows, :] = value[0:rows]
                lhs[c, k, h, 0:rows, :] = lax.dot_general(
                    pick, value[-rows:], (((0,), (0,)), ((), ())), preferred_element_type=f32
                ).astype(bf16)

        def packed(c, k, b):
            return remote(
                pack_out.at[c, k, b], pack_in.at[c, k, b], pack_send.at[k, c, b], pack_recv.at[k, c, b], partner
            )

        def go_down(p):
            c, g, first, many = passes[p]
            band = pl.ds(first * rows, many * rows)
            if p not in loaded:
                heard(p)
                activate(p)
            if "down" not in loaded:
                down_load.wait()
                loaded.add("down")
            k = 0 if g == 0 else 1 + first

            def deliver(f, made):
                at = spans[f]
                h, (low, wide) = f // 2, subs[f % 2]
                if within and g == 0:
                    acc[c, :, at] = arrived[c, :, at].astype(f32) + made[0:rows]
                    ret_send[c, 0, :, at] = made[rows:].astype(bf16)
                    go(back_to_mate(c, f))
                elif within:
                    for j in range(2):
                        opp_made[c, j, :, at] = made[j * rows : (j + 1) * rows]
                else:
                    if g == 0:
                        acc[c, :, at] = arrived[c, :, at].astype(f32) + made[rows:]
                    local = pl.ds(low, wide)
                    pack_out[c, k, h, :, local] = made[0:8].astype(bf16)
                    if h == 0:
                        spare[c, k, :, local] = made[8:16]
                    else:
                        pack_out[c, k, 2, :, local] = (spare[c, k, :, local] + made[8:16]).astype(bf16)
                    if f == 1:
                        go(packed(c, k, 0))
                    if f == 3:
                        go(packed(c, k, 2))
                        go(packed(c, k, 1))

            last = None
            for f, at in enumerate(spans):
                left = active[c, g, band, :] if within else lhs[c, k, f // 2, 0 : many * rows, :]
                made = jnp.dot(left, down[:, at], preferred_element_type=f32)
                if last is not None:
                    deliver(f - 1, last)
                last = made
            deliver(len(spans) - 1, last)

        def spread(c, k, f, pick):
            h, (low, wide) = f // 2, subs[f % 2]
            local = pl.ds(low, wide)
            if f == 0:
                packed(c, k, 0).wait_recv()
                packed(c, k, 2).wait_recv()
            if f == 2:
                packed(c, k, 1).wait_recv()
            got = jnp.concatenate(
                [pack_in[c, k, h, :, local].astype(f32), pack_in[c, k, 2, :, local].astype(f32)], axis=0
            ).astype(bf16)
            return jnp.dot(pick[h], got, preferred_element_type=f32)

        def absorb(c):
            pick = picks(meta[c, 0, 0:rows], mate_id)
            for f, at in enumerate(spans):
                acc[c, :, at] += spread(c, 0, f, pick)

        def back_to_mate(c, f):
            at = spans[f]
            return remote(
                ret_send.at[c, 0, :, at], ret_in.at[c, 0, :, at],
                rets_send.at[0, c, f], rets_recv.at[0, c, f], partner,
            )

        def sum_home(c, f, j):
            at = spans[f]
            return remote(
                ret_send.at[c, 1 + j, :, at], ret_in.at[c, 1, :, at],
                rets_send.at[1 + j, c, f], rets_recv.at[1, c, f], beyond if j else across,
            )

        def combine(c, j):
            pick = picks(meta[c, 1, spot(j)], mate_id)
            for f, at in enumerate(spans):
                ret_send[c, 1 + j, :, at] = (
                    opp_made[c, j, :, at] + spread(c, 1 + j, f, pick)
                ).astype(bf16)
                go(sum_home(c, f, j))

        def finish(c):
            for f, at in enumerate(spans):
                total = acc[c, :, at]
                if not within:
                    back_to_mate(c, f).wait_recv()
                    total += ret_in[c, 0, :, at].astype(f32)
                sum_home(c, f, 0).wait_recv()
                total += ret_in[c, 1, :, at].astype(f32)
                out_ref[heading(c), :, at] = total.astype(bf16)

        near = take_in(0)
        far = take_in(1)
        if within:
            passes = [(0, 0, 0, 2), (0, 1, 0, 2), (1, 0, 0, 2), (1, 1, 0, 2)]
            weigh(0, near)
            relay_rows(0, 0)
            relay_mate(0)
            relay_mate(1)
            relay_mate_tile(0)
            send_across(1, 2, 4)
            weigh(1, far)
            go_up(0)
            relay_rows(0, 1)
            relay_tile(0, 0)
            relay_mate_tile(1)
            go_up(1)
            relay_rows(1, 1)
            relay_tile(0, 1)
            go_up(2)
            relay_tile(1, 1)
            relay_rows(1, 0)
            go_up(3)
            relay_tile(1, 0)
            go_down(1)
            go_down(0)
            go_down(2)
            combine(0, 0)
            go_down(3)
            combine(0, 1)
            combine(1, 1)
            combine(1, 0)
            absorb(0)
            absorb(1)
        else:
            passes = [(0, 0, 0, 2), (1, 0, 0, 2), (0, 1, 0, 1), (0, 1, 1, 1), (1, 1, 1, 1), (1, 1, 0, 1)]
            weigh(0, near)
            go_up(0)
            weigh(1, far)
            go_up(1)
            go_up(2)
            go_down(0)
            go_down(1)
            go_up(3)
            go_down(2)
            go_up(4)
            go_down(3)
            go_up(5)
            go_down(4)
            go_down(5)
        finish(0)
        finish(1)
        for copy in started:
            copy.wait_send()

    @pl.when(inside == 1)
    def _():
        perform(True)

    @pl.when(inside == 0)
    def _():
        perform(False)


def relayed(sizes, stream, expert_ids, norm_gain, router, w_up, w_down):
    n_pipe, n_exp, n_ten = sizes
    rows, width = stream.shape[2:]
    experts, fanout = router.shape[2], expert_ids.shape[3]
    hidden_units = w_up.shape[2]
    cap = 3 * rows * fanout // (2 * experts)
    pieces = 4
    bf16, f32 = jnp.bfloat16, jnp.float32
    dma = pltpu.SemaphoreType.DMA
    vmem = pl.BlockSpec(memory_space=pltpu.VMEM)
    hbm = pl.BlockSpec(memory_space=pl.ANY)
    result = pl.pallas_call(
        functools.partial(relay, sizes, cap),
        out_shape=pltpu.VMEM((2, rows, width), bf16),
        in_specs=[hbm] * 6,
        out_specs=vmem,
        scratch_shapes=[
            pltpu.VMEM((2, fanout, rows), jnp.int32),
            pltpu.VMEM((width, hidden_units), bf16),
            pltpu.VMEM((hidden_units, width), bf16),
            pltpu.VMEM((2, rows, width), bf16),
            pltpu.VMEM((2, rows, width), bf16),
            pltpu.VMEM((2, 2, 2 * rows, width), bf16),
            pltpu.VMEM((2, 2, 2 * rows, hidden_units), f32),
            pltpu.VMEM((2, 2, 2 * rows, hidden_units), bf16),
            pltpu.VMEM((2, 2, 2 * rows, hidden_units), bf16),
            pltpu.VMEM((2, 2, 2 * rows, hidden_units), bf16),
            pltpu.VMEM((2, rows, 128), f32),
            pltpu.VMEM((2, rows, 128), f32),
            pltpu.VMEM((2, 2, 2 * rows, 128), f32),
            pltpu.VMEM((2, rows, width), f32),
            pltpu.VMEM((2, 2, rows, width), f32),
            pltpu.VMEM((2, 3, 2, 2 * rows, hidden_units), bf16),
            pltpu.VMEM((2, 3, 8, width // 2), f32),
            pltpu.VMEM((2, 3, 3, 8, width // 2), bf16),
            pltpu.VMEM((2, 3, 3, 8, width // 2), bf16),
            pltpu.VMEM((2, 3, rows, width), bf16),
            pltpu.VMEM((2, 2, rows, width), bf16),
            pltpu.VMEM((1, width + 1024), f32),
            pltpu.VMEM((experts, width), f32),
            dma((5 + pieces,)),
            dma((2,)),
            dma((2,)),
            dma((5, 2, pieces)),
            dma((3, 2, pieces)),
            dma((8,)),
            dma((8,)),
            dma((5, 2)),
            dma((3, 2)),
            dma((3, 2, pieces)),
            dma((2, 2, pieces)),
            dma((3, 2, 3)),
            dma((3, 2, 3)),
        ],
        compiler_params=pltpu.CompilerParams(
            collective_id=0, has_side_effects=True, vmem_limit_bytes=67043328 - 4 * rows * width - 16384
        ),
    )(stream, expert_ids[:, 0].transpose(0, 2, 1), norm_gain, router[0].T, w_up, w_down)
    return result.reshape(2, 1, rows, width)


def shards(sizes, stream, expert_ids, norm_gain, router, w_up, w_down):
    n_pipe, n_exp, n_ten = sizes
    if n_exp == 4 and n_ten == 2 and n_pipe > 1 and n_pipe % 2 == 0 and router.shape[2] == n_exp:
        return relayed(sizes, stream, expert_ids, norm_gain, router, w_up, w_down)
    tok_rows, width = stream.shape[2:]
    fanout = expert_ids.shape[-1]
    experts = router.shape[2]
    hidden_units = w_up.shape[2]
    tokens = 2 * tok_rows
    capacity = 3 * tok_rows * fanout // (2 * experts)
    slots = -(-2 * capacity // 8) * 8
    total = n_exp * slots
    feat = pieces_of(width, 4)
    cols = pieces_of(hidden_units, 4)
    bf16, f32 = jnp.bfloat16, jnp.float32
    dma = pltpu.SemaphoreType.DMA
    vmem = pl.BlockSpec(memory_space=pltpu.VMEM)
    hbm = pl.BlockSpec(memory_space=pl.ANY)
    result = pl.pallas_call(
        functools.partial(layer, sizes, slots, feat, cols),
        out_shape=jax.ShapeDtypeStruct((tokens, width), bf16),
        in_specs=[hbm, vmem, hbm, vmem, hbm, hbm],
        out_specs=vmem,
        scratch_shapes=[
            pltpu.VMEM((width, hidden_units), bf16),
            pltpu.VMEM((hidden_units, width), bf16),
            pltpu.VMEM((tokens, width), bf16),
            pltpu.VMEM((n_exp, -(-slots // 16) * 16, width), bf16),
            pltpu.VMEM((n_exp, -(-slots // 16) * 16, width), bf16),
            pltpu.VMEM((total, width // feat), f32),
            pltpu.VMEM((total, hidden_units), f32),
            pltpu.VMEM((cols, total, hidden_units // cols), bf16),
            pltpu.VMEM((n_ten, cols, total, hidden_units // cols), bf16),
            pltpu.VMEM((total, hidden_units), bf16),
            pltpu.VMEM((total, 128), f32),
            pltpu.VMEM((n_ten, total, 128), f32),
            pltpu.VMEM((2, tokens, 128), f32),
            pltpu.VMEM((n_ten, 2, tokens, 128), f32),
            pltpu.VMEM((n_exp, -(-slots // 16) * 16, width), bf16),
            pltpu.VMEM((n_exp, -(-slots // 16) * 16, width), bf16),
            pltpu.VMEM((2, tokens, -(-total // 128) * 128), bf16),
            pltpu.VMEM((1, width + 1024), f32),
            dma((feat + 2,)),
            dma((2,)),
            dma((2,)),
            dma((n_exp, feat)),
            dma((n_exp, feat)),
            dma((n_ten, cols + 2)),
            dma((n_ten, cols + 2)),
            dma((n_exp, feat)),
            dma((n_exp, feat)),
        ],
        compiler_params=pltpu.CompilerParams(
            collective_id=0, has_side_effects=True, vmem_limit_bytes=60 * 1024 * 1024
        ),
    )(stream, expert_ids.reshape(tokens, fanout), norm_gain, router[0].T, w_up, w_down)
    return result.reshape(2, 1, tok_rows, width)


def solution(mesh):
    sizes = tuple(mesh.shape[axis] for axis in ("pipe", "expert", "tensor"))
    return jax.shard_map(
        functools.partial(shards, sizes),
        mesh=mesh,
        in_specs=(
            P(None, "pipe", "expert", "tensor"),
            P(None, "pipe", "expert", None),
            P("pipe", "tensor"),
            P("pipe", "tensor", None),
            P("expert", "tensor", None),
            P("expert", None, "tensor"),
        ),
        out_specs=P(None, "pipe", "expert", "tensor"),
        check_vma=False,
    )
```
